32 devices in a mesh: grp: 4 (over x, core), fsdp: 8 (over z, y).
Axes of the slice: x: 2, y: 2, z: 4, core: 2. Of those that a mesh axis runs over, the one named last changes fastest.
Arguments:
- layer_input_rows: bfloat16 [16384, 8192], P(('grp', 'fsdp')), may hold values from -400 to 400, as said below
- input_norm_gain: bfloat16 [8192], replicated, may hold values from 0.5 to 1.5
- key_value_codes: int32 [8192, 256], P('fsdp'), may hold values from 0 to 65535
- block_scale_codes: int32 [256, 128], P('fsdp'), may hold values from -2147483648 to 2147483646
- outer_scale_codes: int32 [512], P('fsdp'), may hold values from 0 to 255
- adapter_down_factor: bfloat16 [8192, 64], replicated, may hold values from -0.0625 to 0.0625
- adapter_up_factor: bfloat16 [64, 1024], replicated, may hold values from -0.75 to 0.75
- target: bfloat16 [16384, 1024], P(('grp', 'fsdp')), may hold values from -18 to 18
Outputs:
- kv: bfloat16 [16384, 1024], P(('grp', 'fsdp'))
- loss: float32 [], replicated
The draws below stay inside these ranges and needn't reach their ends.
Inputs may be any that keep to these rules, and one draw needn't show every extreme that they name: layer_input_rows rows and features carry varied scales.
All inputs are finite; a program needn't handle non-finite values.
Results may differ from the reference program's by a relative error of at most 0.0057.
Values may be sent and summed in bfloat16 or wider, within the bound.
A program may use at most 128 MiB of HBM per device.

```python
import jax
import jax.numpy as jnp
from jax import lax

MODEL_WIDTH = 8192
ADAPTER_RANK = 64
KEY_VALUE_COLS = 1024
GROUP_TOKENS = 4096
TOKENS = 16384
N_GRP = 4


def draw_layer_input_rows(key, part):
    key_noise = jax.random.fold_in(key, 11)
    key_rows = jax.random.fold_in(key, 12)
    key_cols = jax.random.fold_in(key, 13)
    row_scale = jnp.exp(jax.random.uniform(key_rows, (TOKENS, 1), jnp.float32) * jnp.log(10.0))
    col_scale = jnp.exp(jax.random.uniform(key_cols, (1, MODEL_WIDTH), jnp.float32) * jnp.log(10.0))
    noise = jnp.clip(jax.random.normal(key_noise, (TOKENS, MODEL_WIDTH), jnp.float32), -4.0, 4.0)
    return (noise * row_scale * col_scale).astype(jnp.bfloat16)


def draw_target(key, part):
    key_noise = jax.random.fold_in(key, 21)
    position = jnp.arange(TOKENS, dtype=jnp.float32) / TOKENS
    growth = 1.0 + 2.0 * position
    noise = jnp.clip(jax.random.normal(key_noise, (TOKENS, KEY_VALUE_COLS), jnp.float32), -6.0, 6.0)
    return (noise * growth[:, None]).astype(jnp.bfloat16)


def set_ends(result, own_key, low, high):
    longest = result.shape.index(max(result.shape))
    spots = []
    for shift in (0, 1):
        where = [jax.random.randint(jax.random.fold_in(own_key, axis), (), 0, length) for axis, length in enumerate(result.shape)]
        where[longest] = (where[longest] + shift) % result.shape[longest]
        spots.append(tuple(where))
    return result.at[spots[0]].set(low).at[spots[1]].set(high)


def centred(rng, dims, deviation, reach, kind=jnp.bfloat16):
    return jnp.clip(deviation * jax.random.normal(rng, dims, jnp.float32), -reach, reach).astype(kind)


def setup_inputs(seed: int = 0) -> dict:
    seeds = jax.random.split(jax.random.key(seed), 9)
    return {
        "layer_input_rows": draw_layer_input_rows(jax.random.fold_in(seeds[8], 71), 0),
        "input_norm_gain": jnp.clip(1.0 + 0.1 * jax.random.normal(seeds[1], (MODEL_WIDTH,), jnp.float32), 0.5, 1.5).astype(jnp.bfloat16),
        "key_value_codes": set_ends(jax.random.randint(seeds[2], (MODEL_WIDTH, KEY_VALUE_COLS // 4), 0, 65536), jax.random.fold_in(seeds[2], 1), 0, 65535).astype(jnp.int32),
        "block_scale_codes": set_ends(jax.random.randint(seeds[3], (MODEL_WIDTH * KEY_VALUE_COLS // 32768, 128), -2147483648, 2147483647), jax.random.fold_in(seeds[3], 1), -2147483648, 2147483646).astype(jnp.int32),
        "outer_scale_codes": set_ends(jax.random.randint(seeds[4], (MODEL_WIDTH * KEY_VALUE_COLS // 16384,), 0, 256), jax.random.fold_in(seeds[4], 1), 0, 255).astype(jnp.int32),
        "adapter_down_factor": centred(seeds[5], (MODEL_WIDTH, ADAPTER_RANK), MODEL_WIDTH ** -0.5, 0.0625),
        "adapter_up_factor": centred(seeds[6], (ADAPTER_RANK, KEY_VALUE_COLS), ADAPTER_RANK ** -0.5, 0.75),
        "target": draw_target(jax.random.fold_in(seeds[8], 71), 0),
    }


adapter_scale = 0.25
epsilon = 1e-06
nf4_levels = (-1.0, -0.6961928009986877, -0.5250730514526367, -0.39491748809814453, -0.28444138169288635, -0.18477343022823334, -0.09105003625154495, 0.0, 0.07958029955625534, 0.16093020141124725, 0.24611230194568634, 0.33791524171066284, 0.44070982933044434, 0.5626170039176941, 0.7229568362236023, 1.0)

def unpack_scales(code_words, outer_scale_codes, all_rows):
    per_row = code_words.size // all_rows
    flat = code_words.reshape(all_rows, per_row)
    shifts = jnp.arange(4, dtype=jnp.int32) * 8
    code_bytes = jnp.bitwise_and(jnp.right_shift(flat[:, :, None], shifts[None, None, :]), 255)
    code_bytes = code_bytes.reshape(all_rows, per_row * 4).astype(jnp.float32)
    group_rows = all_rows // outer_scale_codes.shape[0]
    second = jnp.exp2(outer_scale_codes.astype(jnp.float32) / 128.0 - 6.0)
    second = jnp.repeat(second, group_rows)
    return (code_bytes + 0.5) / 256.0 * second[:, None]

def decode_codes(words, absmax):
    height = words.shape[0]
    shifts = jnp.arange(4, dtype=jnp.int32) * 4
    nibbles = jnp.bitwise_and(jnp.right_shift(words[:, :, None], shifts[None, None, :]), 15)
    nibbles = nibbles.reshape(height, words.shape[1] * 4)
    values = jnp.zeros(nibbles.shape, jnp.float32)
    for number, level in enumerate(nf4_levels):
        values = jnp.where(nibbles == number, jnp.float32(level), values)
    width = values.shape[1]
    count = absmax.shape[1]
    scaled = values.reshape(height, count, width // count) * absmax[:, :, None]
    return scaled.reshape(height, width).astype(jnp.bfloat16)

def apply_input_norm(input_states, input_norm_gain):
    values = input_states.astype(jnp.float32)
    inverse = lax.rsqrt(lax.optimization_barrier(jnp.mean(values * values, axis=1, keepdims=True)) + epsilon)
    return (values * inverse * input_norm_gain.astype(jnp.float32)[None, :]).astype(jnp.bfloat16)

def key_value_project(normed_input, decoded_weight, adapter_down_factor, adapter_up_factor):
    frozen_output = jnp.dot(normed_input, decoded_weight, preferred_element_type=jnp.float32)
    adapter_output = jnp.dot(normed_input, adapter_down_factor, preferred_element_type=jnp.float32).astype(jnp.bfloat16)
    return frozen_output + adapter_scale * jnp.dot(adapter_output, adapter_up_factor, preferred_element_type=jnp.float32)

def reference(layer_input_rows, input_norm_gain, key_value_codes, block_scale_codes, outer_scale_codes, adapter_down_factor, adapter_up_factor, target):
    absmax = unpack_scales(block_scale_codes, outer_scale_codes, key_value_codes.shape[0])
    decoded_weight = decode_codes(key_value_codes, absmax)

    def one_group(pair):
        input_states, teacher = pair
        precise_output = key_value_project(apply_input_norm(input_states, input_norm_gain), decoded_weight, adapter_down_factor, adapter_up_factor)
        error_terms = precise_output - teacher.astype(jnp.float32)
        return (precise_output.astype(jnp.bfloat16), jnp.sum(error_terms * error_terms) / (GROUP_TOKENS * KEY_VALUE_COLS))
    kv_out, losses = lax.map(one_group, (layer_input_rows.reshape(N_GRP, GROUP_TOKENS, MODEL_WIDTH), target.reshape(N_GRP, GROUP_TOKENS, KEY_VALUE_COLS)))
    return (kv_out.reshape(TOKENS, KEY_VALUE_COLS), jnp.sum(losses))
```

```python
import functools

import jax
import jax.numpy as jnp
from jax import lax
from jax.experimental import pallas as pl
from jax.experimental.pallas import tpu as pltpu
from jax.sharding import PartitionSpec as P

adapter_scale = 0.25
epsilon = 1e-06
nf4_levels = (
    -1.0,
    -0.6961928009986877,
    -0.5250730514526367,
    -0.39491748809814453,
    -0.28444138169288635,
    -0.18477343022823334,
    -0.09105003625154495,
    0.0,
    0.07958029955625534,
    0.16093020141124725,
    0.24611230194568634,
    0.33791524171066284,
    0.44070982933044434,
    0.5626170039176941,
    0.7229568362236023,
    1.0,
)
MESH = pl.DeviceIdType.MESH


def nibble_levels(words, plane):
    values = [jnp.float32(level) for level in nf4_levels]
    for bit in range(4):
        is_set = jnp.bitwise_and(words, 1 << (4 * plane + bit)) != 0
        values = [
            jnp.where(is_set, values[2 * i + 1], values[2 * i])
            for i in range(len(values) // 2)
        ]
    return values[0]


def plan(layers, pieces, groups):
    by_z = max(pieces // 2, pieces * 13 // 16)
    by_y = pieces // 2
    own_y = max(pieces // 2, pieces * 14 // 16)
    early = min(3, own_y)
    y_lag, x_lag = 3, 3
    lag = y_lag + x_lag
    group = pieces // groups
    slots = (layers - 1) * by_z
    spare = by_z - by_y
    ready = max(by_z, by_y + lag)
    per = -(-2 * groups // by_z)

    def own_slot(o):
        if o < early:
            return o - early
        return (o - early) // spare * by_z + by_y + (o - early) % spare

    last = (layers - 2) * by_z
    total = max(slots, last + by_y + lag, own_slot(own_y - 1) + y_lag + 1)
    total = max(total, (layers - 3) * by_z + ready + -(-2 * groups // per))

    def seen(kind, i):
        twin = pieces - 1 - i
        if kind == 0:
            return ready
        if kind == 1:
            return own_slot(i) + y_lag if i < own_y else own_slot(twin) + lag
        if kind == 2:
            return last + (i if i < by_z else twin + lag)
        return last + (i + y_lag if i < by_y else twin + lag)

    items = []
    for kind in range(4):
        for g in range(groups):
            when = max(seen(kind, i) for i in range(g * group, (g + 1) * group))
            items.append((when + 2, kind, g))
    items.sort()
    extras, tail, slot = [], [], ready + 9
    for when, kind, g in items:
        slot = max(slot, when)
        if slot < total:
            extras.append((slot, kind, g))
            slot += 1
        else:
            tail.append((kind, g))
    return dict(
        by_z=by_z,
        by_y=by_y,
        own_y=own_y,
        early=early,
        y_lag=y_lag,
        lag=lag,
        group=group,
        slots=slots,
        spare=spare,
        ready=ready,
        per=per,
        total=total,
        extras=extras,
        tail=tail,
    )


def kernel(
    layers,
    pieces,
    groups,
    x_hbm,
    gain_hbm,
    codes_hbm,
    scales_hbm,
    outer_hbm,
    down_hbm,
    up_hbm,
    target_hbm,
    out_ref,
    loss_ref,
    x_ref,
    weight_ref,
    acc_ref,
    target_ref,
    down_ref,
    up_ref,
    gain_ref,
    codes_ref,
    scales_ref,
    outer_ref,
    spread_ref,
    scale_ref,
    wide_gain_ref,
    low_ref,
    plane_ref,
    line_ref,
    local_sem,
    z_send,
    x_send,
    y_send,
    core_send,
    link_recv,
    core_recv,
    plane_send,
    plane_recv,
    line_send,
    line_recv,
):
    g = lax.axis_index("grp")
    f = lax.axis_index("fsdp")
    cx, cc = g // 2, g % 2
    cl, cy = f // 2, f % 2
    tokens, width = x_ref.shape
    columns = acc_ref.shape[1]
    rows = codes_ref.shape[0]
    high = rows // 2 // pieces
    p = plan(layers, pieces, groups)
    by_z, by_y, own_y, early = p["by_z"], p["by_y"], p["own_y"], p["early"]
    y_lag, lag, group, spare = p["y_lag"], p["lag"], p["group"], p["spare"]
    slots, ready = p["slots"], p["ready"]

    sibling = (cx * 2 + 1 - cc, f)
    x_peer = ((1 - cx) * 2 + cc, f)
    y_peer = (g, cl * 2 + 1 - cy)

    def z_peer(step):
        return (g, (cl + step) * 2 + cy)

    def inside(layer):
        return (layer >= 0) & (layer < layers)

    barrier = pltpu.get_barrier_semaphore()
    for peer in (x_peer, y_peer, sibling):
        pl.semaphore_signal(barrier, inc=1, device_id=peer, device_id_type=MESH)
    for step in (-1, 1):

        @pl.when(inside(cl + step))
        def _():
            pl.semaphore_signal(barrier, inc=1, device_id=z_peer(step), device_id_type=MESH)

    part = tokens // 4
    scales_copy = pltpu.make_async_copy(scales_hbm, scales_ref, local_sem.at[6])
    outer_copy = pltpu.make_async_copy(outer_hbm, outer_ref, local_sem.at[7])
    codes_copy = pltpu.make_async_copy(codes_hbm, codes_ref, local_sem.at[8])
    gain_copy = pltpu.make_async_copy(gain_hbm, gain_ref, local_sem.at[9])
    up_copy = pltpu.make_async_copy(up_hbm, up_ref, local_sem.at[10])
    target_copy = pltpu.make_async_copy(target_hbm, target_ref, local_sem.at[4])
    down_copy = pltpu.make_async_copy(down_hbm, down_ref, local_sem.at[5])

    def x_copy(i):
        at = pl.ds(pl.multiple_of(i * part, part), part)
        return pltpu.make_async_copy(x_hbm.at[at], x_ref.at[at], local_sem.at[i])

    scales_copy.start()
    outer_copy.start()
    codes_copy.start()
    gain_copy.start()
    for i in range(4):
        x_copy(i).start()
    down_copy.start()
    up_copy.start()
    target_copy.start()

    spot = (cx * 2 + cc) * 2 + cy

    def plane_peer(i):
        to = (spot + i) % 8
        return (to // 2, cl * 2 + to % 2)

    def line_peer(i):
        return (g, (cl + i) % layers * 2 + cy)

    def mirror(px, j):
        return j + px * (pieces - 1 - 2 * j)

    def chunk(layer, y, c, q):
        start = (layer * 2 + y) * rows + (q * 2 + c) * high
        return weight_ref.at[pl.ds(pl.multiple_of(start, high), high)]

    def slot(layer, y, q):
        return (layer * 2 + y) * pieces + q

    def link_copy(layer, y, q, send_sem, peer):
        ref = chunk(layer, y, cc, q)
        return pltpu.make_async_remote_copy(
            src_ref=ref,
            dst_ref=ref,
            send_sem=send_sem,
            recv_sem=link_recv.at[slot(layer, y, q)],
            device_id=peer,
            device_id_type=MESH,
        )

    def z_copy(layer, j, step):
        sem = z_send.at[(1 + step) // 2 * layers + layer]
        return link_copy(layer, cy, mirror(cx, j), sem, z_peer(step))

    def x_piece(layer, y, j):
        return link_copy(layer, y, mirror(cx, j), x_send.at[layer], x_peer)

    def y_piece(layer, j):
        return link_copy(layer, cy, mirror(cx, j), y_send.at[layer], y_peer)

    def core_copy(layer, y, q):
        ref = chunk(layer, y, cc, q)
        return pltpu.make_async_remote_copy(
            src_ref=ref,
            dst_ref=ref,
            send_sem=core_send.at[layer * 2 + y],
            recv_sem=core_recv.at[(layer * 2 + y) * groups + q // group],
            device_id=sibling,
            device_id_type=MESH,
        )

    def landed(ref, sem):
        pltpu.make_async_copy(ref, ref, sem).wait()

    def arrived(layer, y, q):
        landed(chunk(layer, y, cc, q), link_recv.at[slot(layer, y, q)])

    def some_rows(count):
        return weight_ref.at[pl.ds(0, count * high)]

    deep = lax.broadcasted_iota(jnp.int32, spread_ref.shape, 0)
    wide = lax.broadcasted_iota(jnp.int32, spread_ref.shape, 1)
    spread_ref[...] = jnp.where(
        (deep % 128) * 4 + deep // 128 == wide, 1.0, 0.0
    ).astype(jnp.bfloat16)

    words = codes_ref.shape[1]
    lanes = scales_ref.shape[1]
    per_row = scales_ref.shape[0] * lanes // rows
    line = rows // scales_ref.shape[0]
    row = lax.broadcasted_iota(jnp.int32, (rows, lanes), 0)
    lane = lax.broadcasted_iota(jnp.int32, (rows, lanes), 1)
    mine = lane // per_row == row % line
    place = lax.broadcasted_iota(jnp.int32, (lanes, words), 0)
    word = lax.broadcasted_iota(jnp.int32, (lanes, words), 1)
    run = words // (4 * per_row)
    code = jnp.zeros((rows, words), jnp.float32)
    scales_copy.wait()
    scale_words = jnp.concatenate(
        [
            jnp.broadcast_to(scales_ref[pl.ds(i, 1), :], (line, lanes))
            for i in range(scales_ref.shape[0])
        ],
        axis=0,
    )
    for byte in range(4):
        value = jnp.bitwise_and(jnp.right_shift(scale_words, 8 * byte), 255)
        value = jnp.where(mine, value.astype(jnp.float32), 0.0).astype(jnp.bfloat16)
        pick = (place % per_row == word // (4 * run)) & ((word // run) % 4 == byte)
        code += jnp.dot(
            value,
            jnp.where(pick, 1.0, 0.0).astype(jnp.bfloat16),
            preferred_element_type=jnp.float32,
        )
    outer_copy.wait()
    outer_count = outer_ref.shape[1]
    outer_rows = rows // outer_count
    outer_row = lax.broadcasted_iota(jnp.int32, (rows, outer_count), 0)
    outer_lane = lax.broadcasted_iota(jnp.int32, (rows, outer_count), 1)
    second = jnp.sum(
        jnp.where(
            outer_row // outer_rows == outer_lane, outer_ref[...].astype(jnp.float32), 0.0
        ),
        axis=1,
        keepdims=True,
    )
    second = jnp.exp2(second / 128.0 - 6.0)
    scale_ref[...] = (code + 0.5) / 256.0 * second

    def decode(c, index):
        starts = [
            pl.multiple_of(((index * group + i) * 2 + c) * high, high) for i in range(group)
        ]
        for h in range(words // 128):
            span = pl.ds(h * 128, 128)
            code_words = jnp.concatenate([codes_ref[pl.ds(s, high), span] for s in starts])
            scale = jnp.concatenate([scale_ref[pl.ds(s, high), span] for s in starts])
            planes = [
                (nibble_levels(code_words, plane) * scale).astype(jnp.bfloat16)
                for plane in range(4)
            ]
            ordered = jnp.dot(
                jnp.concatenate(planes, axis=1),
                spread_ref[...],
                preferred_element_type=jnp.float32,
            ).astype(jnp.bfloat16)
            for i, s in enumerate(starts):
                weight_ref[
                    pl.ds(pl.multiple_of(f * rows + s, high), high), pl.ds(h * 512, 512)
                ] = ordered[i * high : (i + 1) * high]

    def turned(index):
        return index + cx * (groups - 1 - 2 * index)

    def own_sends(index):
        for i in range(group):
            j = index * group + i
            for step in (-1, 1):

                @pl.when(inside(cl + step) & (j < by_z))
                def _():
                    z_copy(cl, j, step).start()

            pl.when(j < early)(lambda: y_piece(cl, j).start())

    codes_copy.wait()
    decode(cc, turned(0))
    neighbours = 3 + jnp.where(cl > 0, 1, 0) + jnp.where(cl < layers - 1, 1, 0)
    pl.semaphore_wait(barrier, neighbours)
    own_sends(0)

    def rest(index, carry):
        decode(cc, turned(index))
        own_sends(index)
        return carry

    lax.fori_loop(1, groups, rest, 0)
    gain_copy.wait()
    wide_gain_ref[...] = gain_ref[...].astype(jnp.float32)

    block = min(16, part)
    blocks = tokens // block
    tile = min(1024, width)

    def normalize(i):
        pl.when(i % (blocks // 4) == 0)(lambda: x_copy(i // (blocks // 4)).wait())
        at = pl.ds(pl.multiple_of(i * block, block), block)
        total = jnp.zeros((block, 128), jnp.float32)
        for t in range(width // tile):
            v = x_ref[at, pl.ds(t * tile, tile)].astype(jnp.float32)
            v = v * v
            for k in range(tile // 128):
                total += v[:, k * 128 : (k + 1) * 128]
        inverse = lax.rsqrt(jnp.sum(total, axis=1, keepdims=True) / width + epsilon)
        for t in range(width // 128):
            span = pl.ds(t * 128, 128)
            v = x_ref[at, span].astype(jnp.float32)
            x_ref[at, span] = (v * inverse * wide_gain_ref[pl.ds(t, 1), :]).astype(jnp.bfloat16)

    def adapter(step):
        at = pl.ds(pl.multiple_of(step * (width // 8), width // 8), width // 8)
        partial = lax.dot_general(
            x_ref[:, at],
            down_ref[:, at],
            (((1,), (1,)), ((), ())),
            preferred_element_type=jnp.float32,
        )

        @pl.when(step == 0)
        def _():
            low_ref[...] = partial

        @pl.when(step > 0)
        def _():
            low_ref[...] += partial

    def adapter_up():
        up_copy.wait()

        acc_ref[...] += adapter_scale * jnp.dot(
            low_ref[...].astype(jnp.bfloat16), up_ref[...], preferred_element_type=jnp.float32
        )

    def multiply(layer, y, index, is_own):
        size = rows // groups

        @pl.when(jnp.logical_not(is_own))
        def _():
            landed(some_rows(group), core_recv.at[(layer * 2 + y) * groups + index])

        at = pl.ds(pl.multiple_of((layer * 2 + y) * rows + index * size, size), size)
        acc_ref[...] += jnp.dot(
            x_ref[:, at], weight_ref[at, :], preferred_element_type=jnp.float32
        )

    shorter = jnp.minimum(cl, layers - 1 - cl)
    longer = jnp.where(cl * 2 < layers - 1, 1, -1)

    def layer_of(v):
        near = v <= 2 * shorter
        away = jnp.where(near, (v + 1) // 2, v - shorter)
        side = jnp.where(near & (v % 2 == 0), -longer, longer)
        return jnp.clip(cl + side * away, 0, layers - 1)

    def stage(k):
        k = jnp.maximum(k, 0)
        return lax.div(k, by_z) + 1, lax.rem(k, by_z)

    def z_event(s, j):
        q = mirror(cx, j)
        for step in (-1, 1):
            layer = cl + step * s

            @pl.when(inside(layer))
            def _():
                arrived(layer, cy, q)
                pl.when(inside(cl - step))(lambda: z_copy(layer, j, -step).start())
                core_copy(layer, cy, q).start()

    def own_index(v, j):
        return early + (v - 1) * spare + j - by_y

    def send_event(v, j):
        layer = layer_of(v)
        pl.when(j < pieces - by_z)(lambda: x_piece(layer, cy, j).start())
        pl.when(j < by_y)(lambda: y_piece(layer, j).start())
        o = own_index(v, j)
        pl.when((j >= by_y) & (o < own_y))(lambda: y_piece(cl, o).start())

    def y_event(k):
        v, j = stage(k)
        o = jnp.where(k < 0, k + early, own_index(v, j))
        moving = (k >= 0) & (j < by_y)
        layer = jnp.where(moving, layer_of(v), cl)
        i = jnp.where(moving, j, o)

        @pl.when(moving | (o < own_y))
        def _():
            q = mirror(cx, i)
            arrived(layer, 1 - cy, q)
            pl.when(moving | (o < pieces - own_y))(
                lambda: x_piece(layer, 1 - cy, i).start()
            )
            core_copy(layer, 1 - cy, q).start()

    def x_event(k):
        v, j = stage(k)
        moving = (k >= 0) & (j < by_y)
        o = k + early
        layer = jnp.where(k < 0, cl, layer_of(v))
        i = jnp.where(k < 0, o, j)
        q = mirror(1 - cx, i)

        @pl.when((k >= 0) & (j < pieces - by_z))
        def _():
            arrived(layer, cy, q)
            core_copy(layer, cy, q).start()

        @pl.when(moving | ((k < 0) & (o < pieces - own_y)))
        def _():
            arrived(layer, 1 - cy, q)
            core_copy(layer, 1 - cy, q).start()

    first = ready - 1
    each = -(-blocks // first)

    def early_work(k):
        def some(i, carry):
            normalize(i)
            return carry

        lax.fori_loop(jnp.minimum(k * each, blocks), jnp.minimum((k + 1) * each, blocks), some, 0)
        often = first // groups
        pl.when((lax.rem(k, often) == 0) & (k < groups * often))(
            lambda: decode(1 - cc, lax.div(k, often))
        )

        @pl.when(k == first - 1)
        def _():
            acc_ref[...] = jnp.zeros(acc_ref.shape, jnp.float32)
            down_copy.wait()

    def extra_of(kind):
        layer = jnp.where(kind < 2, cl, layer_of(layers - 1))
        y = jnp.where(kind % 2 == 0, cy, 1 - cy)
        return layer, y

    def late_work(k):
        past = k - ready
        v, j = stage(past)
        for i in range(p["per"]):
            index = j * p["per"] + i

            @pl.when((v < layers - 1) & (index < 2 * groups))
            def _():
                y = jnp.where(index < groups, cy, 1 - cy)
                multiply(layer_of(v), y, turned(index % groups), False)

        pl.when(past < 8)(lambda: adapter(past))
        pl.when(past == 8)(adapter_up)

        @pl.when(past > 8)
        def _():
            kind, index = jnp.int32(-1), jnp.int32(0)
            for when, a, b in p["extras"]:
                kind = jnp.where(k == when, a, kind)
                index = jnp.where(k == when, b, index)

            @pl.when(kind >= 0)
            def _():
                layer, y = extra_of(kind)
                multiply(layer, y, turned(index), kind == 0)

    def one_slot(k, carry):
        @pl.when(k < slots)
        def _():
            v, j = stage(k)
            z_event(v, j)
            send_event(v, j)

        pl.when(k >= y_lag - early)(lambda: y_event(k - y_lag))
        pl.when(k >= lag - early)(lambda: x_event(k - lag))
        pl.when(k < first)(lambda: early_work(k))
        pl.when(k >= ready)(lambda: late_work(k))
        return carry

    lax.fori_loop(0, p["total"], one_slot, 0)
    for kind, index in p["tail"]:
        layer, y = extra_of(jnp.int32(kind))
        multiply(layer, y, turned(index), kind == 0)

    target_copy.wait()
    plane_ref[spot] = jnp.zeros((8, 128), jnp.float32)

    def finish(i, carry):
        at = pl.ds(pl.multiple_of(i * block, block), block)
        exact = acc_ref[at, :]
        out_ref[at, :] = exact.astype(jnp.bfloat16)
        error = exact - target_ref[at, :].astype(jnp.float32)
        error = error * error
        total = jnp.zeros((block, 128), jnp.float32)
        for k in range(columns // 128):
            total += error[:, k * 128 : (k + 1) * 128]
        for k in range(block // 8):
            plane_ref[spot] += total[k * 8 : (k + 1) * 8]
        return carry

    lax.fori_loop(0, tokens // block, finish, 0)

    def plane_copy(i):
        return pltpu.make_async_remote_copy(
            src_ref=plane_ref.at[spot],
            dst_ref=plane_ref.at[spot],
            send_sem=plane_send.at[i],
            recv_sem=plane_recv.at[spot],
            device_id=plane_peer(i),
            device_id_type=MESH,
        )

    def line_copy(i):
        return pltpu.make_async_remote_copy(
            src_ref=line_ref.at[cl],
            dst_ref=line_ref.at[cl],
            send_sem=line_send.at[i],
            recv_sem=line_recv.at[cl],
            device_id=line_peer(i),
            device_id_type=MESH,
        )

    for i in range(1, 8):
        plane_copy(i).start()

    def sent(layer, carry):
        for step in (-1, 1):

            @pl.when(inside(cl + step) & ((cl - layer) * step >= 0))
            def _():
                landed(some_rows(by_z), z_send.at[(1 + step) // 2 * layers + layer])

        @pl.when(layer == cl)
        def _():
            landed(some_rows(own_y), y_send.at[layer])
            landed(some_rows(pieces - own_y), x_send.at[layer])

        @pl.when(layer != cl)
        def _():
            landed(some_rows(by_y), y_send.at[layer])
            landed(some_rows(pieces - by_z + by_y), x_send.at[layer])
            landed(some_rows(pieces), core_send.at[layer * 2 + cy])

        landed(some_rows(pieces), core_send.at[layer * 2 + 1 - cy])
        return carry

    lax.fori_loop(0, layers, sent, 0)
    for i in range(1, 8):
        source = (spot + i) % 8
        landed(plane_ref.at[source], plane_recv.at[source])
    line_ref[cl] = jnp.sum(plane_ref[...], axis=0)

    def to_line(i, carry):
        line_copy(i).start()
        return carry

    def from_line(i, carry):
        source = (cl + i) % layers
        landed(line_ref.at[source], line_recv.at[source])
        line_copy(i).wait_send()
        return carry

    lax.fori_loop(1, layers, to_line, 0)
    for i in range(1, 8):
        plane_copy(i).wait_send()
    lax.fori_loop(1, layers, from_line, 0)
    loss_ref[0, 0] = jnp.sum(line_ref[...]) / (tokens * layers * 2 * columns)


def per_device(fsdp, x, gain, codes, scales, outer, down, up, target):
    tokens, width = x.shape
    columns = up.shape[1]
    rows = codes.shape[0]
    layers = fsdp // 2
    pieces = rows // 2 // max(16, rows // 32)
    groups = min(4, rows // 128)
    hbm = pl.BlockSpec(memory_space=pltpu.HBM)
    dma = pltpu.SemaphoreType.DMA
    gain = gain.reshape(-1, 128)
    outer = outer.reshape(1, -1)
    operands = (x, gain, codes, scales, outer, down.T, up, target)
    operands = [pltpu.with_memory_space_constraint(a, pltpu.HBM) for a in operands]
    kv, loss = pl.pallas_call(
        functools.partial(kernel, layers, pieces, groups),
        out_shape=(
            jax.ShapeDtypeStruct((tokens, columns), jnp.bfloat16),
            jax.ShapeDtypeStruct((1, 1), jnp.float32),
        ),
        in_specs=[hbm] * 8,
        out_specs=(
            pl.BlockSpec(memory_space=pltpu.VMEM),
            pl.BlockSpec(memory_space=pltpu.SMEM),
        ),
        scratch_shapes=[
            pltpu.VMEM((tokens, width), jnp.bfloat16),
            pltpu.VMEM((width, columns), jnp.bfloat16),
            pltpu.VMEM((tokens, columns), jnp.float32),
            pltpu.VMEM((tokens, columns), jnp.bfloat16),
            pltpu.VMEM(down.shape[::-1], jnp.bfloat16),
            pltpu.VMEM(up.shape, jnp.bfloat16),
            pltpu.VMEM(gain.shape, jnp.bfloat16),
            pltpu.VMEM(codes.shape, jnp.int32),
            pltpu.VMEM(scales.shape, jnp.int32),
            pltpu.VMEM(outer.shape, jnp.int32),
            pltpu.VMEM((512, 512), jnp.bfloat16),
            pltpu.VMEM(codes.shape, jnp.float32),
            pltpu.VMEM((width // 128, 128), jnp.float32),
            pltpu.VMEM((tokens, down.shape[1]), jnp.float32),
            pltpu.VMEM((8, 8, 128), jnp.float32),
            pltpu.VMEM((layers, 8, 128), jnp.float32),
            dma((11,)),
            dma((2 * layers,)),
            dma((layers,)),
            dma((layers,)),
            dma((2 * layers,)),
            dma((layers * 2 * pieces,)),
            dma((layers * 2 * groups,)),
            dma((8,)),
            dma((8,)),
            dma((layers,)),
            dma((layers,)),
        ],
        compiler_params=pltpu.CompilerParams(
            collective_id=0, has_side_effects=True, vmem_limit_bytes=40 * 1024 * 1024
        ),
    )(*operands)
    return kv, loss.reshape(())


def solution(mesh):
    placed = (
        P(("grp", "fsdp"), None),
        P(),
        P("fsdp", None),
        P("fsdp", None),
        P("fsdp"),
        P(),
        P(),
        P(("grp", "fsdp"), None),
    )
    return jax.shard_map(
        functools.partial(per_device, mesh.shape["fsdp"]),
        mesh=mesh,
        in_specs=placed,
        out_specs=(P(("grp", "fsdp"), None), P()),
        check_vma=False,
    )
```

```python
import functools

import jax
import jax.numpy as jnp
from jax import lax
from jax.experimental import pallas as pl
from jax.experimental.pallas import tpu as pltpu
from jax.sharding import PartitionSpec as P

adapter_scale = 0.25
epsilon = 1e-06
nf4_levels = (
    -1.0,
    -0.6961928009986877,
    -0.5250730514526367,
    -0.39491748809814453,
    -0.28444138169288635,
    -0.18477343022823334,
    -0.09105003625154495,
    0.0,
    0.07958029955625534,
    0.16093020141124725,
    0.24611230194568634,
    0.33791524171066284,
    0.44070982933044434,
    0.5626170039176941,
    0.7229568362236023,
    1.0,
)
MESH = pl.DeviceIdType.MESH
FAR, OWN, EARLY, YLAG, XLAG = 0, 14, 4, 4, 3


def nibble_levels(words, plane):
    values = [jnp.float32(level) for level in nf4_levels]
    for bit in range(4):
        is_set = jnp.bitwise_and(words, 1 << (4 * plane + bit)) != 0
        values = [
            jnp.where(is_set, values[2 * i + 1], values[2 * i])
            for i in range(len(values) // 2)
        ]
    return values[0]


def plan(layers, pieces, groups, blocks):
    by_z = max(pieces // 2, pieces * 13 // 16)
    far = max(pieces // 2, by_z - pieces // 16 * FAR)
    by_y = pieces // 2
    own_y = pieces * OWN // 16
    early = min(EARLY, own_y)
    y_lag, x_lag = YLAG, XLAG
    lag = y_lag + x_lag
    group = pieces // groups
    spare = by_z - by_y
    turn = (layers - 3) * by_z + by_y
    slots = turn + by_z + far - by_y
    ready = max(by_z, by_y + lag)
    per = -(-2 * groups // by_z)
    each = -(-blocks // (ready - 1))
    normal = -(-blocks // each)

    def own_slot(o):
        if o < early:
            return o - early
        o -= early
        if o < (layers - 3) * spare:
            return o // spare * by_z + by_y + o % spare
        return turn + by_y + o - (layers - 3) * spare

    def z_slot(hop, i):
        if hop == layers - 1:
            return turn + i if i < by_y else turn + by_z + i - by_y
        if hop == layers - 2:
            return (layers - 3) * by_z + i if i < by_y else turn + i
        return (hop - 1) * by_z + i

    def send_slot(v, i):
        return turn + i if v == layers - 1 else (v - 1) * by_z + i

    last_x = turn + by_y + y_lag
    total = max(slots, last_x + x_lag + pieces - far, own_slot(own_y - 1) + y_lag + 1)
    total = max(total, (layers - 4) * by_z + ready + -(-2 * groups // per))

    def seen(kind, i):
        twin = pieces - 1 - i
        if kind == 0:
            return normal - 1
        if kind == 1:
            return own_slot(i) + y_lag if i < own_y else own_slot(twin) + lag
        v = layers - 1 - (kind - 2) // 2
        if kind % 2 == 0:
            when = 0
            for shorter in range((layers + 1) // 2):
                hop = (v + 1) // 2 if v <= 2 * shorter else v - shorter
                count = far if hop == layers - 1 else by_z
                over = last_x + x_lag + twin if v == layers - 1 else send_slot(v, twin) + lag
                when = max(when, z_slot(hop, i) if i < count else over)
            return when
        return send_slot(v, i) + y_lag if i < by_y else send_slot(v, twin) + lag

    items = []
    for kind in range(6):
        for g in range(groups):
            when = max(seen(kind, i) for i in range(g * group, (g + 1) * group))
            items.append((max(when + 2, normal), kind, g))
    items.sort()
    extras, tail = [], []
    taken = {}
    for when, kind, g in items:
        slot = when
        while ready <= slot < ready + 9 or taken.get(slot, 0) >= (1 if slot < turn + by_y else 2):
            slot += 1
        taken[slot] = taken.get(slot, 0) + 1
        if slot < slots - 1:
            extras.append((slot, taken[slot], kind, g))
        else:
            tail.append((kind, g))
    return dict(
        by_z=by_z,
        far=far,
        by_y=by_y,
        own_y=own_y,
        early=early,
        y_lag=y_lag,
        lag=lag,
        group=group,
        turn=turn,
        last_x=last_x,
        x_lag=x_lag,
        slots=slots,
        spare=spare,
        ready=ready,
        per=per,
        each=each,
        normal=normal,
        total=total,
        extras=extras,
        tail=tail,
    )


def kernel(
    layers,
    pieces,
    groups,
    x_hbm,
    gain_hbm,
    codes_hbm,
    scales_hbm,
    outer_hbm,
    down_hbm,
    up_hbm,
    target_hbm,
    out_ref,
    loss_ref,
    x_ref,
    weight_ref,
    acc_ref,
    target_ref,
    down_ref,
    up_ref,
    gain_ref,
    codes_ref,
    scales_ref,
    outer_ref,
    spread_ref,
    pick_ref,
    scale_ref,
    wide_gain_ref,
    low_ref,
    share_ref,
    losses_ref,
    local_sem,
    z_send,
    x_send,
    y_send,
    core_send,
    link_recv,
    core_recv,
    loss_sem,
):
    g = lax.axis_index("grp")
    f = lax.axis_index("fsdp")
    cx, cc = g // 2, g % 2
    cl, cy = f // 2, f % 2
    tokens, width = x_ref.shape
    columns = acc_ref.shape[1]
    rows = codes_ref.shape[0]
    high = rows // 2 // pieces
    block = min(16, tokens // 4)
    blocks = tokens // block
    p = plan(layers, pieces, groups, blocks)
    by_z, by_y, own_y, early = p["by_z"], p["by_y"], p["own_y"], p["early"]
    y_lag, lag, group, spare = p["y_lag"], p["lag"], p["group"], p["spare"]
    slots, ready, far, turn = p["slots"], p["ready"], p["far"], p["turn"]

    sibling = (cx * 2 + 1 - cc, f)
    x_peer = ((1 - cx) * 2 + cc, f)
    y_peer = (g, cl * 2 + 1 - cy)

    def z_peer(step):
        return (g, (cl + step) * 2 + cy)

    def by_hop(h):
        return jnp.where(h == layers - 1, far, by_z)

    def inside(layer):
        return (layer >= 0) & (layer < layers)

    barrier = pltpu.get_barrier_semaphore()
    for peer in (x_peer, y_peer, sibling):
        pl.semaphore_signal(barrier, inc=1, device_id=peer, device_id_type=MESH)
    for step in (-1, 1):

        @pl.when(inside(cl + step))
        def _():
            pl.semaphore_signal(barrier, inc=1, device_id=z_peer(step), device_id_type=MESH)

    part = tokens // 4
    scales_copy = pltpu.make_async_copy(scales_hbm, scales_ref, local_sem.at[6])
    outer_copy = pltpu.make_async_copy(outer_hbm, outer_ref, local_sem.at[7])
    codes_copy = pltpu.make_async_copy(codes_hbm, codes_ref, local_sem.at[8])
    gain_copy = pltpu.make_async_copy(gain_hbm, gain_ref, local_sem.at[9])
    up_copy = pltpu.make_async_copy(up_hbm, up_ref, local_sem.at[10])
    target_copy = pltpu.make_async_copy(target_hbm, target_ref, local_sem.at[4])
    down_copy = pltpu.make_async_copy(down_hbm, down_ref, local_sem.at[5])

    def x_copy(i):
        at = pl.ds(pl.multiple_of(i * part, part), part)
        return pltpu.make_async_copy(x_hbm.at[at], x_ref.at[at], local_sem.at[i])

    scales_copy.start()
    outer_copy.start()
    codes_copy.start()
    gain_copy.start()
    for i in range(4):
        x_copy(i).start()
    down_copy.start()
    up_copy.start()
    target_copy.start()

    def mirror(px, j):
        return j + px * (pieces - 1 - 2 * j)

    def chunk(layer, y, c, q):
        start = (layer * 2 + y) * rows + (q * 2 + c) * high
        return weight_ref.at[pl.ds(pl.multiple_of(start, high), high)]

    def slot(layer, y, q):
        return (layer * 2 + y) * pieces + q

    def link_copy(layer, y, q, send_sem, peer):
        ref = chunk(layer, y, cc, q)
        return pltpu.make_async_remote_copy(
            src_ref=ref,
            dst_ref=ref,
            send_sem=send_sem,
            recv_sem=link_recv.at[slot(layer, y, q)],
            device_id=peer,
            device_id_type=MESH,
        )

    def z_copy(layer, j, step):
        sem = z_send.at[(1 + step) // 2 * layers + layer]
        return link_copy(layer, cy, mirror(cx, j), sem, z_peer(step))

    def x_piece(layer, y, j):
        return link_copy(layer, y, mirror(cx, j), x_send.at[layer], x_peer)

    def y_piece(layer, j):
        return link_copy(layer, cy, mirror(cx, j), y_send.at[layer], y_peer)

    def core_copy(layer, y, q):
        ref = chunk(layer, y, cc, q)
        return pltpu.make_async_remote_copy(
            src_ref=ref,
            dst_ref=ref,
            send_sem=core_send.at[layer * 2 + y],
            recv_sem=core_recv.at[(layer * 2 + y) * groups + q // group],
            device_id=sibling,
            device_id_type=MESH,
        )

    def landed(ref, sem):
        pltpu.make_async_copy(ref, ref, sem).wait()

    def arrived(layer, y, q):
        landed(chunk(layer, y, cc, q), link_recv.at[slot(layer, y, q)])

    def some_rows(count):
        return weight_ref.at[pl.ds(0, count * high)]

    deep = lax.broadcasted_iota(jnp.int32, spread_ref.shape, 0)
    wide = lax.broadcasted_iota(jnp.int32, spread_ref.shape, 1)
    spread_ref[...] = jnp.where(
        (deep % 128) * 4 + deep // 128 == wide, 1.0, 0.0
    ).astype(jnp.bfloat16)

    words = codes_ref.shape[1]
    lanes = scales_ref.shape[1]
    per_row = scales_ref.shape[0] * lanes // rows
    line = rows // scales_ref.shape[0]
    run = words // (4 * per_row)
    bunch = rows // groups
    lines = scales_ref.shape[0] // groups
    place = lax.broadcasted_iota(jnp.int32, pick_ref.shape, 0)
    word = lax.broadcasted_iota(jnp.int32, pick_ref.shape, 1)
    pick = (place % per_row == word // (4 * run)) & ((word // run) % 4 == place // lanes)
    pick_ref[...] = jnp.where(pick, 1.0, 0.0).astype(jnp.bfloat16)
    row = lax.broadcasted_iota(jnp.int32, (bunch, lanes), 0)
    lane = lax.broadcasted_iota(jnp.int32, (bunch, lanes), 1)
    mine = lane // per_row == row % line
    outer_count = outer_ref.shape[1]
    outer_rows = rows // outer_count
    outer_row = lax.broadcasted_iota(jnp.int32, (bunch, outer_count), 0) // outer_rows
    outer_lane = lax.broadcasted_iota(jnp.int32, (bunch, outer_count), 1)

    def unpack(index):
        scale_words = jnp.concatenate(
            [
                jnp.broadcast_to(scales_ref[pl.ds(index * lines + i, 1), :], (line, lanes))
                for i in range(lines)
            ],
            axis=0,
        )
        values = []
        for byte in range(4):
            value = jnp.bitwise_and(jnp.right_shift(scale_words, 8 * byte), 255)
            values.append(jnp.where(mine, value.astype(jnp.float32), 0.0).astype(jnp.bfloat16))
        code = jnp.dot(
            jnp.concatenate(values, axis=1), pick_ref[...], preferred_element_type=jnp.float32
        )
        mask = outer_row + index * (bunch // outer_rows) == outer_lane
        second = jnp.sum(
            jnp.where(mask, outer_ref[...].astype(jnp.float32), 0.0), axis=1, keepdims=True
        )
        second = jnp.exp2(second / 128.0 - 6.0)
        at = pl.ds(pl.multiple_of(index * bunch, bunch), bunch)
        scale_ref[at, :] = (code + 0.5) / 256.0 * second

    def decode(c, index):
        starts = [
            pl.multiple_of(((index * group + i) * 2 + c) * high, high) for i in range(group)
        ]
        for h in range(words // 128):
            span = pl.ds(h * 128, 128)
            code_words = jnp.concatenate([codes_ref[pl.ds(s, high), span] for s in starts])
            scale = jnp.concatenate([scale_ref[pl.ds(s, high), span] for s in starts])
            planes = [
                (nibble_levels(code_words, plane) * scale).astype(jnp.bfloat16)
                for plane in range(4)
            ]
            ordered = jnp.dot(
                jnp.concatenate(planes, axis=1),
                spread_ref[...],
                preferred_element_type=jnp.float32,
            ).astype(jnp.bfloat16)
            for i, s in enumerate(starts):
                weight_ref[
                    pl.ds(pl.multiple_of(f * rows + s, high), high), pl.ds(h * 512, 512)
                ] = ordered[i * high : (i + 1) * high]

    def turned(index):
        return index + cx * (groups - 1 - 2 * index)

    def own_sends(index):
        for i in range(group):
            j = index * group + i
            for step in (-1, 1):

                @pl.when(inside(cl + step) & (j < by_hop(1)))
                def _():
                    z_copy(cl, j, step).start()

            pl.when(j < early)(lambda: y_piece(cl, j).start())

    scales_copy.wait()
    outer_copy.wait()
    unpack(turned(0))
    codes_copy.wait()
    decode(cc, turned(0))
    neighbours = 3 + jnp.where(cl > 0, 1, 0) + jnp.where(cl < layers - 1, 1, 0)
    pl.semaphore_wait(barrier, neighbours)
    own_sends(0)

    def rest(index, carry):
        unpack(turned(index))
        decode(cc, turned(index))
        own_sends(index)
        return carry

    lax.fori_loop(1, groups, rest, 0)
    gain_copy.wait()
    wide_gain_ref[...] = gain_ref[...].astype(jnp.float32)

    tile = min(1024, width)

    def normalize(i):
        pl.when(i % (blocks // 4) == 0)(lambda: x_copy(i // (blocks // 4)).wait())
        at = pl.ds(pl.multiple_of(i * block, block), block)
        total = jnp.zeros((block, 128), jnp.float32)
        for t in range(width // tile):
            v = x_ref[at, pl.ds(t * tile, tile)].astype(jnp.float32)
            v = v * v
            for k in range(tile // 128):
                total += v[:, k * 128 : (k + 1) * 128]
        inverse = lax.rsqrt(jnp.sum(total, axis=1, keepdims=True) / width + epsilon)
        for t in range(width // 128):
            span = pl.ds(t * 128, 128)
            v = x_ref[at, span].astype(jnp.float32)
            x_ref[at, span] = (v * inverse * wide_gain_ref[pl.ds(t, 1), :]).astype(jnp.bfloat16)

    def adapter(step):
        at = pl.ds(pl.multiple_of(step * (width // 8), width // 8), width // 8)
        partial = lax.dot_general(
            x_ref[:, at],
            down_ref[:, at],
            (((1,), (1,)), ((), ())),
            preferred_element_type=jnp.float32,
        )

        @pl.when(step == 0)
        def _():
            low_ref[...] = partial

        @pl.when(step > 0)
        def _():
            low_ref[...] += partial

    def adapter_up():
        up_copy.wait()

        acc_ref[...] += adapter_scale * jnp.dot(
            low_ref[...].astype(jnp.bfloat16), up_ref[...], preferred_element_type=jnp.float32
        )

    def multiply(layer, y, index, is_own):
        size = rows // groups

        @pl.when(jnp.logical_not(is_own))
        def _():
            landed(some_rows(group), core_recv.at[(layer * 2 + y) * groups + index])

        at = pl.ds(pl.multiple_of((layer * 2 + y) * rows + index * size, size), size)
        acc_ref[...] += jnp.dot(
            x_ref[:, at], weight_ref[at, :], preferred_element_type=jnp.float32
        )

    shorter = jnp.minimum(cl, layers - 1 - cl)
    longer = jnp.where(cl * 2 < layers - 1, 1, -1)

    def hops_of(v):
        return jnp.where(v <= 2 * shorter, (v + 1) // 2, v - shorter)

    def layer_of(v):
        near = v <= 2 * shorter
        away = hops_of(v)
        side = jnp.where(near & (v % 2 == 0), -longer, longer)
        return jnp.clip(cl + side * away, 0, layers - 1)

    def stage(k):
        k = jnp.maximum(k, 0)
        return lax.div(k, by_z) + 1, lax.rem(k, by_z)

    def z_stage(k):
        s, j = stage(k)
        past = k - turn
        s = jnp.where(past >= 0, layers - 1, s)
        j = jnp.where(past >= 0, past, j)
        second = (past >= by_y) & (past < by_z)
        s = jnp.where(second, layers - 2, s)
        j = jnp.where(past >= by_z, past - by_z + by_y, j)
        return s, j

    def send_stage(k):
        v, j = stage(k)
        past = k - turn
        return jnp.where(past >= 0, layers - 1, v), jnp.where(past >= 0, past, j)

    def held(hop, j):
        return (hop == layers - 3) & (j >= by_y)

    def z_event(k):
        s, j = z_stage(k)
        q = mirror(cx, j)
        late = k - (layers - 3) * by_z
        for step in (-1, 1):
            layer = cl + step * s

            @pl.when(inside(layer) & (j < by_hop(s)))
            def _():
                arrived(layer, cy, q)
                go = inside(cl - step) & (j < by_hop(s + 1)) & jnp.logical_not(held(s, j))
                pl.when(go)(lambda: z_copy(layer, j, -step).start())
                core_copy(layer, cy, q).start()

            if layers > 3:
                layer_held = cl + step * (layers - 3)
                waiting = (late >= by_y) & (late < by_z) & (late < by_hop(layers - 2))

                @pl.when(waiting & inside(layer_held) & inside(cl - step))
                def _():
                    z_copy(layer_held, late, -step).start()

    def own_index(v, j):
        v = jnp.minimum(v, layers - 2)
        return early + (v - 1) * spare + j - by_y

    def send_event(k):
        v, j = send_stage(k)
        layer = layer_of(v)
        pl.when((v < layers - 1) & (j < pieces - by_hop(hops_of(v))))(
            lambda: x_piece(layer, cy, j).start()
        )
        pl.when(j < by_y)(lambda: y_piece(layer, j).start())
        o = own_index(v, j)
        pl.when((j >= by_y) & (o < own_y))(lambda: y_piece(cl, o).start())

    def y_event(k):
        v, j = send_stage(k)
        o = jnp.where(k < 0, k + early, own_index(v, j))
        moving = (k >= 0) & (j < by_y)
        layer = jnp.where(moving, layer_of(v), cl)
        i = jnp.where(moving, j, o)

        @pl.when(moving | (o < own_y))
        def _():
            q = mirror(cx, i)
            arrived(layer, 1 - cy, q)
            pl.when(moving | (o < pieces - own_y))(
                lambda: x_piece(layer, 1 - cy, i).start()
            )
            core_copy(layer, 1 - cy, q).start()

    def x_event(k):
        v, j = send_stage(k)
        moving = (k >= 0) & (j < by_y)
        o = k + early
        layer = jnp.where(k < 0, cl, layer_of(v))
        i = jnp.where(k < 0, o, j)
        q = mirror(1 - cx, i)

        @pl.when((k >= 0) & (v < layers - 1) & (j < pieces - by_hop(hops_of(v))))
        def _():
            arrived(layer, cy, q)
            core_copy(layer, cy, q).start()

        @pl.when(moving | ((k < 0) & (o < pieces - own_y)))
        def _():
            arrived(layer, 1 - cy, q)
            core_copy(layer, 1 - cy, q).start()

    def last_x_event(k):
        v = layers - 1
        layer = layer_of(v)
        count = pieces - by_hop(hops_of(v))
        j = k - p["last_x"]
        pl.when((j >= 0) & (j < count))(lambda: x_piece(layer, cy, j).start())
        i = j - p["x_lag"]

        @pl.when((i >= 0) & (i < count))
        def _():
            q = mirror(1 - cx, i)
            arrived(layer, cy, q)
            core_copy(layer, cy, q).start()

    each = p["each"]
    often = max(1, (p["normal"] - 1) // groups)

    def early_work(k):
        def some(i, carry):
            normalize(i)
            return carry

        lax.fori_loop(jnp.minimum(k * each, blocks), jnp.minimum((k + 1) * each, blocks), some, 0)
        pl.when((lax.rem(k, often) == 0) & (k < groups * often))(
            lambda: decode(1 - cc, lax.div(k, often))
        )

        @pl.when(k == p["normal"] - 1)
        def _():
            acc_ref[...] = jnp.zeros(acc_ref.shape, jnp.float32)
            down_copy.wait()

    def extra_of(kind):
        layer = layer_of(layers - 1 - lax.div(jnp.maximum(kind - 2, 0), 2))
        layer = jnp.where(kind < 2, cl, layer)
        y = jnp.where(lax.rem(kind, 2) == 0, cy, 1 - cy)
        return layer, y

    def extra_work(k):
        for order in (1, 2):
            chosen = [e for e in p["extras"] if e[1] == order]

            @pl.when(k >= min([e[0] for e in chosen], default=p["total"]))
            def _():
                choice = jnp.int32(-1)
                for when, _, a, b in chosen:
                    choice = jnp.where(k == when, a * groups + b, choice)

                @pl.when(choice >= 0)
                def _():
                    kind, index = lax.div(choice, groups), lax.rem(choice, groups)
                    layer, y = extra_of(kind)
                    multiply(layer, y, turned(index), kind == 0)

    def late_work(k):
        past = k - ready
        v, j = stage(past)
        for i in range(p["per"]):
            index = j * p["per"] + i

            @pl.when((v < layers - 2) & (index < 2 * groups))
            def _():
                y = jnp.where(index < groups, cy, 1 - cy)
                multiply(layer_of(v), y, turned(lax.rem(index, groups)), False)

        pl.when(past < 8)(lambda: adapter(past))
        pl.when(past == 8)(adapter_up)

    def one_slot(k, carry):
        @pl.when(k < slots)
        def _():
            z_event(k)
            send_event(k)

        pl.when(k >= y_lag - early)(lambda: y_event(k - y_lag))
        pl.when(k >= lag - early)(lambda: x_event(k - lag))
        pl.when(k >= p["last_x"])(lambda: last_x_event(k))
        pl.when(k < p["normal"])(lambda: early_work(k))
        pl.when(k >= ready)(lambda: late_work(k))
        extra_work(k)
        return carry

    lax.fori_loop(0, p["total"], one_slot, 0)
    for kind, index in p["tail"]:
        layer, y = extra_of(jnp.int32(kind))
        multiply(layer, y, turned(index), kind == 0)

    target_copy.wait()
    share_ref[...] = jnp.zeros((8, 128), jnp.float32)

    def finish(i, carry):
        at = pl.ds(pl.multiple_of(i * block, block), block)
        exact = acc_ref[at, :]
        out_ref[at, :] = exact.astype(jnp.bfloat16)
        error = exact - target_ref[at, :].astype(jnp.float32)
        error = error * error
        total = jnp.zeros((block, 128), jnp.float32)
        for k in range(columns // 128):
            total += error[:, k * 128 : (k + 1) * 128]
        for k in range(block // 8):
            share_ref[...] += total[k * 8 : (k + 1) * 8]
        return carry

    lax.fori_loop(0, tokens // block, finish, 0)

    fsdp = layers * 2
    members = 4 * fsdp
    spot = g * fsdp + f
    losses_ref[spot] = jnp.sum(share_ref[...], axis=0, keepdims=True)

    def tell(j, carry):
        to = f + j
        to = jnp.where(to >= fsdp, to - fsdp, to)
        for i in range(4):

            @pl.when((i > 0) | (j > 0))
            def _():
                pltpu.make_async_remote_copy(
                    src_ref=losses_ref.at[spot],
                    dst_ref=losses_ref.at[spot],
                    send_sem=loss_sem.at[0],
                    recv_sem=loss_sem.at[1],
                    device_id=((g + i) % 4, to),
                    device_id_type=MESH,
                ).start()

        return carry

    lax.fori_loop(0, fsdp, tell, 0)

    def sent(layer, carry):
        hops = jnp.abs(cl - layer)
        for step in (-1, 1):

            for count, test in ((far, hops == layers - 2), (by_z, hops < layers - 2)):

                @pl.when(inside(cl + step) & ((cl - layer) * step >= 0) & test)
                def _():
                    landed(some_rows(count), z_send.at[(1 + step) // 2 * layers + layer])

        @pl.when(layer == cl)
        def _():
            landed(some_rows(own_y), y_send.at[layer])
            if own_y < pieces:
                landed(some_rows(pieces - own_y), x_send.at[layer])

        @pl.when(layer != cl)
        def _():
            landed(some_rows(by_y), y_send.at[layer])
            for count, test in ((far, hops == layers - 1), (by_z, hops < layers - 1)):
                pl.when(test)(
                    lambda: landed(some_rows(pieces - count + by_y), x_send.at[layer])
                )
            landed(some_rows(pieces), core_send.at[layer * 2 + cy])

        landed(some_rows(pieces), core_send.at[layer * 2 + 1 - cy])
        return carry

    lax.fori_loop(0, layers, sent, 0)
    others = losses_ref.at[pl.ds(0, members - 1)]
    landed(others, loss_sem.at[1])
    everyone = jnp.sum(losses_ref[...], axis=0)
    loss_ref[...] = jnp.sum(everyone, axis=1, keepdims=True) / (tokens * fsdp * columns)
    landed(others, loss_sem.at[0])


def per_device(fsdp, x, gain, codes, scales, outer, down, up, target):
    tokens, width = x.shape
    columns = up.shape[1]
    rows = codes.shape[0]
    layers = fsdp // 2
    pieces = rows // 2 // max(16, rows // 32)
    groups = min(4, rows // 128)
    hbm = pl.BlockSpec(memory_space=pltpu.HBM)
    dma = pltpu.SemaphoreType.DMA
    gain = gain.reshape(-1, 128)
    outer = outer.reshape(1, -1)
    operands = (x, gain, codes, scales, outer, down.T, up, target)
    operands = [pltpu.with_memory_space_constraint(a, pltpu.HBM) for a in operands]
    kv, loss = pl.pallas_call(
        functools.partial(kernel, layers, pieces, groups),
        out_shape=(
            jax.ShapeDtypeStruct((tokens, columns), jnp.bfloat16),
            jax.ShapeDtypeStruct((1, 1), jnp.float32),
        ),
        in_specs=[hbm] * 8,
        out_specs=(
            pl.BlockSpec(memory_space=pltpu.VMEM),
            pl.BlockSpec(memory_space=pltpu.VMEM),
        ),
        scratch_shapes=[
            pltpu.VMEM((tokens, width), jnp.bfloat16),
            pltpu.VMEM((width, columns), jnp.bfloat16),
            pltpu.VMEM((tokens, columns), jnp.float32),
            pltpu.VMEM((tokens, columns), jnp.bfloat16),
            pltpu.VMEM(down.shape[::-1], jnp.bfloat16),
            pltpu.VMEM(up.shape, jnp.bfloat16),
            pltpu.VMEM(gain.shape, jnp.bfloat16),
            pltpu.VMEM(codes.shape, jnp.int32),
            pltpu.VMEM(scales.shape, jnp.int32),
            pltpu.VMEM(outer.shape, jnp.int32),
            pltpu.VMEM((512, 512), jnp.bfloat16),
            pltpu.VMEM((4 * scales.shape[1], codes.shape[1]), jnp.bfloat16),
            pltpu.VMEM(codes.shape, jnp.float32),
            pltpu.VMEM((width // 128, 128), jnp.float32),
            pltpu.VMEM((tokens, down.shape[1]), jnp.float32),
            pltpu.VMEM((8, 128), jnp.float32),
            pltpu.VMEM((4 * fsdp, 1, 128), jnp.float32),
            dma((11,)),
            dma((2 * layers,)),
            dma((layers,)),
            dma((layers,)),
            dma((2 * layers,)),
            dma((layers * 2 * pieces,)),
            dma((layers * 2 * groups,)),
            dma((2,)),
        ],
        compiler_params=pltpu.CompilerParams(
            collective_id=0, has_side_effects=True, vmem_limit_bytes=40 * 1024 * 1024
        ),
    )(*operands)
    return kv, loss.reshape(())


def solution(mesh):
    placed = (
        P(("grp", "fsdp"), None),
        P(),
        P("fsdp", None),
        P("fsdp", None),
        P("fsdp"),
        P(),
        P(),
        P(("grp", "fsdp"), None),
    )
    return jax.shard_map(
        functools.partial(per_device, mesh.shape["fsdp"]),
        mesh=mesh,
        in_specs=placed,
        out_specs=(P(("grp", "fsdp"), None), P()),
        check_vma=False,
    )
```

```python
import functools

import jax
import jax.numpy as jnp
from jax import lax
from jax.experimental import pallas as pl
from jax.experimental.pallas import tpu as pltpu
from jax.sharding import PartitionSpec as P

adapter_scale = 0.25
epsilon = 1e-06
nf4_levels = (
    -1.0,
    -0.6961928009986877,
    -0.5250730514526367,
    -0.39491748809814453,
    -0.28444138169288635,
    -0.18477343022823334,
    -0.09105003625154495,
    0.0,
    0.07958029955625534,
    0.16093020141124725,
    0.24611230194568634,
    0.33791524171066284,
    0.44070982933044434,
    0.5626170039176941,
    0.7229568362236023,
    1.0,
)
MESH = pl.DeviceIdType.MESH
OWN, EARLY, YLAG, XLAG = 14, 4, 4, 3


def nibble_levels(words, plane):
    values = [jnp.float32(level) for level in nf4_levels]
    for bit in range(4):
        is_set = jnp.bitwise_and(words, 1 << (4 * plane + bit)) != 0
        values = [
            jnp.where(is_set, values[2 * i + 1], values[2 * i])
            for i in range(len(values) // 2)
        ]
    return values[0]


def plan(layers, pieces, groups, blocks):
    by_z = max(pieces // 2, pieces * 13 // 16)
    by_y = pieces // 2
    own_y = pieces * OWN // 16
    early = min(EARLY, own_y)
    y_lag, x_lag = YLAG, XLAG
    lag = y_lag + x_lag
    group = pieces // groups
    spare = by_z - by_y
    turn = (layers - 3) * by_z + by_y
    slots = turn + by_z + by_z - by_y
    ready = max(by_z, by_y + lag)
    per = -(-2 * groups // by_z)
    each = -(-blocks // (ready - 1))
    normal = -(-blocks // each)

    def own_slot(o):
        if o < early:
            return o - early
        o -= early
        if o < (layers - 3) * spare:
            return o // spare * by_z + by_y + o % spare
        return turn + by_y + o - (layers - 3) * spare

    def z_slot(hop, i):
        if hop == layers - 1:
            return turn + i if i < by_y else turn + by_z + i - by_y
        if hop == layers - 2:
            return (layers - 3) * by_z + i if i < by_y else turn + i
        return (hop - 1) * by_z + i

    def send_slot(v, i):
        return turn + i if v == layers - 1 else (v - 1) * by_z + i

    last_x = turn + by_y + y_lag
    total = max(slots, last_x + x_lag + pieces - by_z, own_slot(own_y - 1) + y_lag + 1)
    total = max(total, (layers - 4) * by_z + ready + -(-2 * groups // per))

    def seen(kind, i):
        twin = pieces - 1 - i
        if kind == 0:
            return normal - 1
        if kind == 1:
            return own_slot(i) + y_lag if i < own_y else own_slot(twin) + lag
        v = layers - 1 - (kind - 2) // 2
        if kind % 2 == 0:
            when = 0
            for shorter in range((layers + 1) // 2):
                hop = (v + 1) // 2 if v <= 2 * shorter else v - shorter
                over = last_x + x_lag + twin if v == layers - 1 else send_slot(v, twin) + lag
                when = max(when, z_slot(hop, i) if i < by_z else over)
            return when
        return send_slot(v, i) + y_lag if i < by_y else send_slot(v, twin) + lag

    items = []
    for kind in range(6):
        for g in range(groups):
            when = max(seen(kind, i) for i in range(g * group, (g + 1) * group))
            items.append((max(when + 2, normal), kind, g))
    items.sort()
    extras, tail = [], []
    taken = {}
    for when, kind, g in items:
        slot = when
        while ready <= slot < ready + 9 or taken.get(slot, 0) >= (1 if slot < turn + by_y else 2):
            slot += 1
        taken[slot] = taken.get(slot, 0) + 1
        if slot < slots - 1:
            extras.append((slot, taken[slot], kind, g))
        else:
            tail.append((kind, g))
    return dict(
        by_z=by_z,
        by_y=by_y,
        own_y=own_y,
        early=early,
        y_lag=y_lag,
        lag=lag,
        group=group,
        turn=turn,
        last_x=last_x,
        x_lag=x_lag,
        slots=slots,
        spare=spare,
        ready=ready,
        per=per,
        each=each,
        normal=normal,
        total=total,
        extras=extras,
        tail=tail,
    )


def kernel(
    layers,
    pieces,
    groups,
    x_hbm,
    gain_hbm,
    codes_hbm,
    scales_hbm,
    outer_hbm,
    down_hbm,
    up_hbm,
    target_hbm,
    out_ref,
    loss_ref,
    x_ref,
    weight_ref,
    acc_ref,
    target_ref,
    down_ref,
    up_ref,
    gain_ref,
    codes_ref,
    scales_ref,
    outer_ref,
    spread_ref,
    pick_ref,
    scale_ref,
    wide_gain_ref,
    low_ref,
    losses_ref,
    local_sem,
    z_send,
    x_send,
    y_send,
    core_send,
    link_recv,
    core_recv,
    loss_sem,
):
    g = lax.axis_index("grp")
    f = lax.axis_index("fsdp")
    cx, cc = g // 2, g % 2
    cl, cy = f // 2, f % 2
    tokens, width = x_ref.shape
    columns = acc_ref.shape[1]
    rows = codes_ref.shape[0]
    high = rows // 2 // pieces
    block = min(16, tokens // 4)
    blocks = tokens // block
    p = plan(layers, pieces, groups, blocks)
    by_z, by_y, own_y, early = p["by_z"], p["by_y"], p["own_y"], p["early"]
    y_lag, lag, group, spare = p["y_lag"], p["lag"], p["group"], p["spare"]
    slots, ready, turn = p["slots"], p["ready"], p["turn"]

    sibling = (cx * 2 + 1 - cc, f)
    x_peer = ((1 - cx) * 2 + cc, f)
    y_peer = (g, cl * 2 + 1 - cy)

    def z_peer(step):
        return (g, (cl + step) * 2 + cy)

    def inside(layer):
        return (layer >= 0) & (layer < layers)

    barrier = pltpu.get_barrier_semaphore()
    for peer in (x_peer, y_peer, sibling):
        pl.semaphore_signal(barrier, inc=1, device_id=peer, device_id_type=MESH)
    for step in (-1, 1):

        @pl.when(inside(cl + step))
        def _():
            pl.semaphore_signal(barrier, inc=1, device_id=z_peer(step), device_id_type=MESH)

    part = tokens // 4
    scales_copy = pltpu.make_async_copy(scales_hbm, scales_ref, local_sem.at[6])
    outer_copy = pltpu.make_async_copy(outer_hbm, outer_ref, local_sem.at[7])
    codes_copy = pltpu.make_async_copy(codes_hbm, codes_ref, local_sem.at[8])
    gain_copy = pltpu.make_async_copy(gain_hbm, gain_ref, local_sem.at[9])
    up_copy = pltpu.make_async_copy(up_hbm, up_ref, local_sem.at[10])
    target_copy = pltpu.make_async_copy(target_hbm, target_ref, local_sem.at[4])
    down_copy = pltpu.make_async_copy(down_hbm, down_ref, local_sem.at[5])

    def x_copy(i):
        at = pl.ds(pl.multiple_of(i * part, part), part)
        return pltpu.make_async_copy(x_hbm.at[at], x_ref.at[at], local_sem.at[i])

    scales_copy.start()
    outer_copy.start()
    codes_copy.start()
    gain_copy.start()
    for i in range(4):
        x_copy(i).start()
    down_copy.start()
    up_copy.start()
    target_copy.start()

    def mirror(px, j):
        return j + px * (pieces - 1 - 2 * j)

    def chunk(layer, y, c, q):
        start = (layer * 2 + y) * rows + (q * 2 + c) * high
        return weight_ref.at[pl.ds(pl.multiple_of(start, high), high)]

    def mine_slot(at, layer, q):
        return jnp.where(layer > at, layer - 1, layer) * pieces + q

    def other_slot(layer, q):
        return (layers - 1 + layer) * pieces + q

    def slot(layer, y, q):
        return jnp.where(y == cy, mine_slot(cl, layer, q), other_slot(layer, q))

    def link_copy(layer, y, q, place, send_sem, peer):
        ref = chunk(layer, y, cc, q)
        return pltpu.make_async_remote_copy(
            src_ref=ref,
            dst_ref=ref,
            send_sem=send_sem,
            recv_sem=link_recv.at[place],
            device_id=peer,
            device_id_type=MESH,
        )

    def z_copy(layer, j, step):
        sem = z_send.at[jnp.where((layer == cl) & (step > 0), layers, layer)]
        q = mirror(cx, j)
        return link_copy(layer, cy, q, mine_slot(cl + step, layer, q), sem, z_peer(step))

    def x_piece(layer, y, j):
        q = mirror(cx, j)
        return link_copy(layer, y, q, slot(layer, y, q), x_send.at[0], x_peer)

    def y_piece(layer, j):
        q = mirror(cx, j)
        return link_copy(layer, cy, q, other_slot(layer, q), y_send.at[0], y_peer)

    def core_copy(layer, y, q):
        ref = chunk(layer, y, cc, q)
        return pltpu.make_async_remote_copy(
            src_ref=ref,
            dst_ref=ref,
            send_sem=core_send.at[y],
            recv_sem=core_recv.at[(layer * 2 + y) * groups + q // group],
            device_id=sibling,
            device_id_type=MESH,
        )

    def landed(ref, sem):
        pltpu.make_async_copy(ref, ref, sem).wait()

    def arrived(layer, y, q):
        landed(chunk(layer, y, cc, q), link_recv.at[slot(layer, y, q)])

    def some_rows(count):
        return weight_ref.at[pl.ds(0, count * high)]

    deep = lax.broadcasted_iota(jnp.int32, spread_ref.shape, 0)
    wide = lax.broadcasted_iota(jnp.int32, spread_ref.shape, 1)
    spread_ref[...] = jnp.where(
        (deep % 128) * 4 + deep // 128 == wide, 1.0, 0.0
    ).astype(jnp.bfloat16)

    words = codes_ref.shape[1]
    lanes = scales_ref.shape[1]
    per_row = scales_ref.shape[0] * lanes // rows
    line = rows // scales_ref.shape[0]
    run = words // (4 * per_row)
    bunch = rows // groups
    lines = scales_ref.shape[0] // groups
    place = lax.broadcasted_iota(jnp.int32, pick_ref.shape, 0)
    word = lax.broadcasted_iota(jnp.int32, pick_ref.shape, 1)
    pick = (place % per_row == word // (4 * run)) & ((word // run) % 4 == place // lanes)
    pick_ref[...] = jnp.where(pick, 1.0, 0.0).astype(jnp.bfloat16)
    row = lax.broadcasted_iota(jnp.int32, (bunch, lanes), 0)
    lane = lax.broadcasted_iota(jnp.int32, (bunch, lanes), 1)
    mine = lane // per_row == row % line
    outer_count = outer_ref.shape[1]
    outer_rows = rows // outer_count
    outer_row = lax.broadcasted_iota(jnp.int32, (bunch, outer_count), 0) // outer_rows
    outer_lane = lax.broadcasted_iota(jnp.int32, (bunch, outer_count), 1)

    def unpack(index):
        scale_words = jnp.concatenate(
            [
                jnp.broadcast_to(scales_ref[pl.ds(index * lines + i, 1), :], (line, lanes))
                for i in range(lines)
            ],
            axis=0,
        )
        values = []
        for byte in range(4):
            value = jnp.bitwise_and(jnp.right_shift(scale_words, 8 * byte), 255)
            values.append(jnp.where(mine, value.astype(jnp.float32), 0.0).astype(jnp.bfloat16))
        code = jnp.dot(
            jnp.concatenate(values, axis=1), pick_ref[...], preferred_element_type=jnp.float32
        )
        mask = outer_row + index * (bunch // outer_rows) == outer_lane
        second = jnp.sum(
            jnp.where(mask, outer_ref[...].astype(jnp.float32), 0.0), axis=1, keepdims=True
        )
        second = jnp.exp2(second / 128.0 - 6.0)
        at = pl.ds(pl.multiple_of(index * bunch, bunch), bunch)
        scale_ref[at, :] = (code + 0.5) / 256.0 * second

    def decode(c, index):
        starts = [
            pl.multiple_of(((index * group + i) * 2 + c) * high, high) for i in range(group)
        ]
        for h in range(words // 128):
            span = pl.ds(h * 128, 128)
            code_words = jnp.concatenate([codes_ref[pl.ds(s, high), span] for s in starts])
            scale = jnp.concatenate([scale_ref[pl.ds(s, high), span] for s in starts])
            planes = [
                (nibble_levels(code_words, plane) * scale).astype(jnp.bfloat16)
                for plane in range(4)
            ]
            ordered = jnp.dot(
                jnp.concatenate(planes, axis=1),
                spread_ref[...],
                preferred_element_type=jnp.float32,
            ).astype(jnp.bfloat16)
            for i, s in enumerate(starts):
                weight_ref[
                    pl.ds(pl.multiple_of(f * rows + s, high), high), pl.ds(h * 512, 512)
                ] = ordered[i * high : (i + 1) * high]

    def turned(index):
        return index + cx * (groups - 1 - 2 * index)

    def own_sends(index):
        for i in range(group):
            j = index * group + i
            for step in (-1, 1):

                @pl.when(inside(cl + step) & (j < by_z))
                def _():
                    z_copy(cl, j, step).start()

            pl.when(j < early)(lambda: y_piece(cl, j).start())

    scales_copy.wait()
    outer_copy.wait()
    unpack(turned(0))
    codes_copy.wait()
    decode(cc, turned(0))
    neighbours = 3 + jnp.where(cl > 0, 1, 0) + jnp.where(cl < layers - 1, 1, 0)
    pl.semaphore_wait(barrier, neighbours)
    own_sends(0)

    def rest(index, carry):
        unpack(turned(index))
        decode(cc, turned(index))
        own_sends(index)
        return carry

    lax.fori_loop(1, groups, rest, 0)
    gain_copy.wait()
    wide_gain_ref[...] = gain_ref[...].astype(jnp.float32)

    tile = min(1024, width)

    def normalize(i):
        pl.when(i % (blocks // 4) == 0)(lambda: x_copy(i // (blocks // 4)).wait())
        at = pl.ds(pl.multiple_of(i * block, block), block)
        total = jnp.zeros((block, 128), jnp.float32)
        for t in range(width // tile):
            v = x_ref[at, pl.ds(t * tile, tile)].astype(jnp.float32)
            v = v * v
            for k in range(tile // 128):
                total += v[:, k * 128 : (k + 1) * 128]
        inverse = lax.rsqrt(jnp.sum(total, axis=1, keepdims=True) / width + epsilon)
        for t in range(width // 128):
            span = pl.ds(t * 128, 128)
            v = x_ref[at, span].astype(jnp.float32)
            x_ref[at, span] = (v * inverse * wide_gain_ref[pl.ds(t, 1), :]).astype(jnp.bfloat16)

    def adapter(step):
        at = pl.ds(pl.multiple_of(step * (width // 8), width // 8), width // 8)
        partial = lax.dot_general(
            x_ref[:, at],
            down_ref[:, at],
            (((1,), (1,)), ((), ())),
            preferred_element_type=jnp.float32,
        )

        @pl.when(step == 0)
        def _():
            low_ref[...] = partial

        @pl.when(step > 0)
        def _():
            low_ref[...] += partial

    def adapter_up():
        up_copy.wait()

        acc_ref[...] += adapter_scale * jnp.dot(
            low_ref[...].astype(jnp.bfloat16), up_ref[...], preferred_element_type=jnp.float32
        )

    def whole(layer, y, index, is_own):
        @pl.when(jnp.logical_not(is_own))
        def _():
            landed(some_rows(group), core_recv.at[(layer * 2 + y) * groups + index])

    def product(layer, y, index):
        size = rows // groups
        at = pl.ds(pl.multiple_of((layer * 2 + y) * rows + index * size, size), size)
        return jnp.dot(x_ref[:, at], weight_ref[at, :], preferred_element_type=jnp.float32)

    def multiply(layer, y, index, is_own):
        whole(layer, y, index, is_own)
        acc_ref[...] += product(layer, y, index)

    shorter = jnp.minimum(cl, layers - 1 - cl)
    longer = jnp.where(cl * 2 < layers - 1, 1, -1)

    def hops_of(v):
        return jnp.where(v <= 2 * shorter, (v + 1) // 2, v - shorter)

    def layer_of(v):
        near = v <= 2 * shorter
        away = hops_of(v)
        side = jnp.where(near & (v % 2 == 0), -longer, longer)
        return jnp.clip(cl + side * away, 0, layers - 1)

    def stage(k):
        k = jnp.maximum(k, 0)
        return lax.div(k, by_z) + 1, lax.rem(k, by_z)

    def z_stage(k):
        s, j = stage(k)
        past = k - turn
        s = jnp.where(past >= 0, layers - 1, s)
        j = jnp.where(past >= 0, past, j)
        second = (past >= by_y) & (past < by_z)
        s = jnp.where(second, layers - 2, s)
        j = jnp.where(past >= by_z, past - by_z + by_y, j)
        return s, j

    def send_stage(k):
        v, j = stage(k)
        past = k - turn
        return jnp.where(past >= 0, layers - 1, v), jnp.where(past >= 0, past, j)

    def held(hop, j):
        return (hop == layers - 3) & (j >= by_y)

    def z_event(k):
        s, j = z_stage(k)
        q = mirror(cx, j)
        late = k - (layers - 3) * by_z
        for step in (-1, 1):
            layer = cl + step * s

            @pl.when(inside(layer))
            def _():
                arrived(layer, cy, q)
                go = inside(cl - step) & jnp.logical_not(held(s, j))
                pl.when(go)(lambda: z_copy(layer, j, -step).start())
                core_copy(layer, cy, q).start()

            if layers > 3:
                layer_held = cl + step * (layers - 3)
                waiting = (late >= by_y) & (late < by_z)

                @pl.when(waiting & inside(layer_held) & inside(cl - step))
                def _():
                    z_copy(layer_held, late, -step).start()

    def own_index(v, j):
        v = jnp.minimum(v, layers - 2)
        return early + (v - 1) * spare + j - by_y

    def send_event(k):
        v, j = send_stage(k)
        layer = layer_of(v)
        pl.when((v < layers - 1) & (j < pieces - by_z))(
            lambda: x_piece(layer, cy, j).start()
        )
        pl.when(j < by_y)(lambda: y_piece(layer, j).start())
        o = own_index(v, j)
        pl.when((j >= by_y) & (o < own_y))(lambda: y_piece(cl, o).start())

    def y_event(k):
        v, j = send_stage(k)
        o = jnp.where(k < 0, k + early, own_index(v, j))
        moving = (k >= 0) & (j < by_y)
        layer = jnp.where(moving, layer_of(v), cl)
        i = jnp.where(moving, j, o)

        @pl.when(moving | (o < own_y))
        def _():
            q = mirror(cx, i)
            arrived(layer, 1 - cy, q)
            pl.when(moving | (o < pieces - own_y))(
                lambda: x_piece(layer, 1 - cy, i).start()
            )
            core_copy(layer, 1 - cy, q).start()

    def x_event(k):
        v, j = send_stage(k)
        moving = (k >= 0) & (j < by_y)
        o = k + early
        layer = jnp.where(k < 0, cl, layer_of(v))
        i = jnp.where(k < 0, o, j)
        q = mirror(1 - cx, i)

        @pl.when((k >= 0) & (v < layers - 1) & (j < pieces - by_z))
        def _():
            arrived(layer, cy, q)
            core_copy(layer, cy, q).start()

        @pl.when(moving | ((k < 0) & (o < pieces - own_y)))
        def _():
            arrived(layer, 1 - cy, q)
            core_copy(layer, 1 - cy, q).start()

    def last_x_event(k):
        v = layers - 1
        layer = layer_of(v)
        count = pieces - by_z
        j = k - p["last_x"]
        pl.when((j >= 0) & (j < count))(lambda: x_piece(layer, cy, j).start())
        i = j - p["x_lag"]

        @pl.when((i >= 0) & (i < count))
        def _():
            q = mirror(1 - cx, i)
            arrived(layer, cy, q)
            core_copy(layer, cy, q).start()

    each = p["each"]
    often = max(1, (p["normal"] - 1) // groups)

    def early_work(k):
        def some(i, carry):
            normalize(i)
            return carry

        lax.fori_loop(jnp.minimum(k * each, blocks), jnp.minimum((k + 1) * each, blocks), some, 0)
        pl.when((lax.rem(k, often) == 0) & (k < groups * often))(
            lambda: decode(1 - cc, lax.div(k, often))
        )

        @pl.when(k == p["normal"] - 1)
        def _():
            acc_ref[...] = jnp.zeros(acc_ref.shape, jnp.float32)
            down_copy.wait()

    def extra_of(kind):
        layer = layer_of(layers - 1 - lax.div(jnp.maximum(kind - 2, 0), 2))
        layer = jnp.where(kind < 2, cl, layer)
        y = jnp.where(lax.rem(kind, 2) == 0, cy, 1 - cy)
        return layer, y

    def extra_work(k):
        for order in (1, 2):
            chosen = [e for e in p["extras"] if e[1] == order]

            @pl.when(k >= min([e[0] for e in chosen], default=p["total"]))
            def _():
                choice = jnp.int32(-1)
                for when, _, a, b in chosen:
                    choice = jnp.where(k == when, a * groups + b, choice)

                @pl.when(choice >= 0)
                def _():
                    kind, index = lax.div(choice, groups), lax.rem(choice, groups)
                    layer, y = extra_of(kind)
                    multiply(layer, y, turned(index), kind == 0)

    def late_work(k):
        past = k - ready
        v, j = stage(past)
        for i in range(p["per"]):
            index = j * p["per"] + i

            @pl.when((v < layers - 2) & (index < 2 * groups))
            def _():
                y = jnp.where(index < groups, cy, 1 - cy)
                multiply(layer_of(v), y, turned(lax.rem(index, groups)), False)

        pl.when(past < 8)(lambda: adapter(past))
        pl.when(past == 8)(adapter_up)

    def one_slot(k, carry):
        @pl.when(k < slots)
        def _():
            z_event(k)
            send_event(k)

        pl.when(k >= y_lag - early)(lambda: y_event(k - y_lag))
        pl.when(k >= lag - early)(lambda: x_event(k - lag))
        pl.when(k >= p["last_x"])(lambda: last_x_event(k))
        pl.when(k < p["normal"])(lambda: early_work(k))
        pl.when(k >= ready)(lambda: late_work(k))
        extra_work(k)
        return carry

    lax.fori_loop(0, p["total"], one_slot, 0)
    target_copy.wait()
    for kind, index in p["tail"][:-1]:
        layer, y = extra_of(jnp.int32(kind))
        multiply(layer, y, turned(index), kind == 0)
    kind, index = p["tail"][-1]
    layer, y = extra_of(jnp.int32(kind))
    whole(layer, y, turned(index), kind == 0)
    exact = acc_ref[...] + product(layer, y, turned(index))
    out_ref[...] = exact.astype(jnp.bfloat16)
    error = exact - target_ref[...].astype(jnp.float32)
    error = error * error
    total = jnp.zeros((tokens, 128), jnp.float32)
    for k in range(columns // 128):
        total += error[:, k * 128 : (k + 1) * 128]
    share = jnp.zeros((8, 128), jnp.float32)
    for k in range(tokens // 8):
        share += total[k * 8 : (k + 1) * 8]

    fsdp = layers * 2
    members = 4 * fsdp
    spot = g * fsdp + f
    losses_ref[spot] = jnp.sum(share, axis=0, keepdims=True)

    def tell(j, carry):
        to = f + j
        to = jnp.where(to >= fsdp, to - fsdp, to)
        for i in range(4):

            @pl.when((i > 0) | (j > 0))
            def _():
                pltpu.make_async_remote_copy(
                    src_ref=losses_ref.at[spot],
                    dst_ref=losses_ref.at[spot],
                    send_sem=loss_sem.at[0],
                    recv_sem=loss_sem.at[1],
                    device_id=((g + i) % 4, to),
                    device_id_type=MESH,
                ).start()

        return carry

    lax.fori_loop(0, fsdp, tell, 0)

    def sent(layer, carry):
        up = inside(cl + 1) & (layer <= cl)
        down = inside(cl - 1) & (layer >= cl)
        own_up = up & (layer == cl)
        pl.when(own_up)(lambda: landed(some_rows(by_z), z_send.at[layers]))
        pl.when(down | (up & (layer != cl)))(
            lambda: landed(some_rows(by_z), z_send.at[layer])
        )
        return carry

    lax.fori_loop(0, layers, sent, 0)
    away = layers - 1
    landed(some_rows(away * by_y + own_y), y_send.at[0])
    landed(some_rows(away * (by_y + pieces - by_z) + pieces - own_y), x_send.at[0])
    landed(some_rows(away * pieces), core_send.at[cy])
    landed(some_rows(layers * pieces), core_send.at[1 - cy])
    others = losses_ref.at[pl.ds(0, members - 1)]
    landed(others, loss_sem.at[1])
    everyone = jnp.sum(losses_ref[...], axis=0)
    loss_ref[...] = jnp.sum(everyone, axis=1, keepdims=True) / (tokens * fsdp * columns)
    landed(others, loss_sem.at[0])


def per_device(fsdp, x, gain, codes, scales, outer, down, up, target):
    tokens, width = x.shape
    columns = up.shape[1]
    rows = codes.shape[0]
    layers = fsdp // 2
    pieces = rows // 2 // max(16, rows // 32)
    groups = min(4, rows // 128)
    hbm = pl.BlockSpec(memory_space=pltpu.HBM)
    dma = pltpu.SemaphoreType.DMA
    gain = gain.reshape(-1, 128)
    outer = outer.reshape(1, -1)
    operands = (x, gain, codes, scales, outer, down.T, up, target)
    operands = [pltpu.with_memory_space_constraint(a, pltpu.HBM) for a in operands]
    kv, loss = pl.pallas_call(
        functools.partial(kernel, layers, pieces, groups),
        out_shape=(
            pltpu.VMEM((tokens, columns), jnp.bfloat16),
            pltpu.VMEM((1, 1), jnp.float32),
        ),
        in_specs=[hbm] * 8,
        out_specs=(
            pl.BlockSpec(memory_space=pltpu.VMEM),
            pl.BlockSpec(memory_space=pltpu.VMEM),
        ),
        scratch_shapes=[
            pltpu.VMEM((tokens, width), jnp.bfloat16),
            pltpu.VMEM((width, columns), jnp.bfloat16),
            pltpu.VMEM((tokens, columns), jnp.float32),
            pltpu.VMEM((tokens, columns), jnp.bfloat16),
            pltpu.VMEM(down.shape[::-1], jnp.bfloat16),
            pltpu.VMEM(up.shape, jnp.bfloat16),
            pltpu.VMEM(gain.shape, jnp.bfloat16),
            pltpu.VMEM(codes.shape, jnp.int32),
            pltpu.VMEM(scales.shape, jnp.int32),
            pltpu.VMEM(outer.shape, jnp.int32),
            pltpu.VMEM((512, 512), jnp.bfloat16),
            pltpu.VMEM((4 * scales.shape[1], codes.shape[1]), jnp.bfloat16),
            pltpu.VMEM(codes.shape, jnp.float32),
            pltpu.VMEM((width // 128, 128), jnp.float32),
            pltpu.VMEM((tokens, down.shape[1]), jnp.float32),
            pltpu.VMEM((4 * fsdp, 1, 128), jnp.float32),
            dma((11,)),
            dma((layers + 1,)),
            dma((1,)),
            dma((1,)),
            dma((2,)),
            dma(((layers * 2 - 1) * pieces,)),
            dma((layers * 2 * groups,)),
            dma((2,)),
        ],
        compiler_params=pltpu.CompilerParams(
            collective_id=0, has_side_effects=True, vmem_limit_bytes=40 * 1024 * 1024
        ),
    )(*operands)
    return kv, loss.reshape(())


def solution(mesh):
    placed = (
        P(("grp", "fsdp"), None),
        P(),
        P("fsdp", None),
        P("fsdp", None),
        P("fsdp"),
        P(),
        P(),
        P(("grp", "fsdp"), None),
    )
    return jax.shard_map(
        functools.partial(per_device, mesh.shape["fsdp"]),
        mesh=mesh,
        in_specs=placed,
        out_specs=(P(("grp", "fsdp"), None), P()),
        check_vma=False,
    )
```

```python
import functools

import jax
import jax.numpy as jnp
from jax import lax
from jax.experimental import pallas as pl
from jax.experimental.pallas import tpu as pltpu
from jax.sharding import PartitionSpec as P

adapter_scale = 0.25
epsilon = 1e-06
nf4_levels = (
    -1.0,
    -0.6961928009986877,
    -0.5250730514526367,
    -0.39491748809814453,
    -0.28444138169288635,
    -0.18477343022823334,
    -0.09105003625154495,
    0.0,
    0.07958029955625534,
    0.16093020141124725,
    0.24611230194568634,
    0.33791524171066284,
    0.44070982933044434,
    0.5626170039176941,
    0.7229568362236023,
    1.0,
)
MESH = pl.DeviceIdType.MESH
OWN, EARLY, YLAG, XLAG = 14, 4, 4, 3


def nibble_levels(words, plane):
    values = [jnp.float32(level) for level in nf4_levels]
    for bit in range(4):
        is_set = jnp.bitwise_and(words, 1 << (4 * plane + bit)) != 0
        values = [
            jnp.where(is_set, values[2 * i + 1], values[2 * i])
            for i in range(len(values) // 2)
        ]
    return values[0]


def plan(layers, pieces, groups, blocks):
    by_z = max(pieces // 2, pieces * 13 // 16)
    by_y = pieces // 2
    own_y = pieces * OWN // 16
    early = min(EARLY, own_y)
    y_lag, x_lag = YLAG, XLAG
    lag = y_lag + x_lag
    group = pieces // groups
    spare = by_z - by_y
    turn = (layers - 3) * by_z + by_y
    slots = turn + by_z + by_z - by_y
    ready = max(by_z, by_y + lag)
    per = -(-2 * groups // by_z)
    each = -(-blocks // (ready - 1))
    normal = -(-blocks // each)

    def own_slot(o):
        if o < early:
            return o - early
        o -= early
        if o < (layers - 3) * spare:
            return o // spare * by_z + by_y + o % spare
        return turn + by_y + o - (layers - 3) * spare

    def z_slot(hop, i):
        if hop == layers - 1:
            return turn + i if i < by_y else turn + by_z + i - by_y
        if hop == layers - 2:
            return (layers - 3) * by_z + i if i < by_y else turn + i
        return (hop - 1) * by_z + i

    def send_slot(v, i):
        return turn + i if v == layers - 1 else (v - 1) * by_z + i

    last_x = turn + by_y + y_lag
    total = max(slots, last_x + x_lag + pieces - by_z, own_slot(own_y - 1) + y_lag + 1)
    total = max(total, (layers - 4) * by_z + ready + -(-2 * groups // per))

    def seen(kind, i):
        twin = pieces - 1 - i
        if kind == 0:
            return normal - 1
        if kind == 1:
            return own_slot(i) + y_lag if i < own_y else own_slot(twin) + lag
        v = layers - 1 - (kind - 2) // 2
        if kind % 2 == 0:
            when = 0
            for shorter in range((layers + 1) // 2):
                hop = (v + 1) // 2 if v <= 2 * shorter else v - shorter
                over = last_x + x_lag + twin if v == layers - 1 else send_slot(v, twin) + lag
                when = max(when, z_slot(hop, i) if i < by_z else over)
            return when
        return send_slot(v, i) + y_lag if i < by_y else send_slot(v, twin) + lag

    items = []
    for kind in range(6):
        for g in range(groups):
            when = max(seen(kind, i) for i in range(g * group, (g + 1) * group))
            when += 1 if when >= slots - 4 else 2
            items.append((max(when, normal), kind, g))
    items.sort()
    extras, tail = [], []
    taken = {}
    for when, kind, g in items:
        slot = when
        while ready <= slot < ready + 9 or taken.get(slot, 0) >= (1 if slot < turn + by_y else 2):
            slot += 1
        taken[slot] = taken.get(slot, 0) + 1
        if slot < slots - 1:
            extras.append((slot, taken[slot], kind, g))
        else:
            tail.append((kind, g))
    return dict(
        by_z=by_z,
        by_y=by_y,
        own_y=own_y,
        early=early,
        y_lag=y_lag,
        lag=lag,
        group=group,
        turn=turn,
        last_x=last_x,
        x_lag=x_lag,
        slots=slots,
        spare=spare,
        ready=ready,
        per=per,
        each=each,
        normal=normal,
        total=total,
        extras=extras,
        tail=tail,
    )


def kernel(
    layers,
    pieces,
    groups,
    x_hbm,
    gain_hbm,
    codes_hbm,
    scales_hbm,
    outer_hbm,
    down_hbm,
    up_hbm,
    target_hbm,
    out_ref,
    loss_ref,
    x_ref,
    weight_ref,
    acc_ref,
    target_ref,
    down_ref,
    up_ref,
    gain_ref,
    codes_ref,
    scales_ref,
    outer_ref,
    spread_ref,
    pick_ref,
    scale_ref,
    wide_gain_ref,
    low_ref,
    losses_ref,
    local_sem,
    z_send,
    x_send,
    y_send,
    core_send,
    link_recv,
    core_recv,
    loss_sem,
):
    g = lax.axis_index("grp")
    f = lax.axis_index("fsdp")
    cx, cc = g // 2, g % 2
    cl, cy = f // 2, f % 2
    tokens, width = x_ref.shape
    columns = acc_ref.shape[1]
    rows = codes_ref.shape[0]
    high = rows // 2 // pieces
    block = min(16, tokens // 4)
    blocks = tokens // block
    p = plan(layers, pieces, groups, blocks)
    by_z, by_y, own_y, early = p["by_z"], p["by_y"], p["own_y"], p["early"]
    y_lag, lag, group, spare = p["y_lag"], p["lag"], p["group"], p["spare"]
    slots, ready, turn = p["slots"], p["ready"], p["turn"]

    sibling = (cx * 2 + 1 - cc, f)
    x_peer = ((1 - cx) * 2 + cc, f)
    y_peer = (g, cl * 2 + 1 - cy)

    def z_peer(step):
        return (g, (cl + step) * 2 + cy)

    def inside(layer):
        return (layer >= 0) & (layer < layers)

    barrier = pltpu.get_barrier_semaphore()
    for peer in (x_peer, y_peer, sibling):
        pl.semaphore_signal(barrier, inc=1, device_id=peer, device_id_type=MESH)
    for step in (-1, 1):

        @pl.when(inside(cl + step))
        def _():
            pl.semaphore_signal(barrier, inc=1, device_id=z_peer(step), device_id_type=MESH)

    part = tokens // 4
    scales_copy = pltpu.make_async_copy(scales_hbm, scales_ref, local_sem.at[6])
    outer_copy = pltpu.make_async_copy(outer_hbm, outer_ref, local_sem.at[7])
    codes_copy = pltpu.make_async_copy(codes_hbm, codes_ref, local_sem.at[8])
    gain_copy = pltpu.make_async_copy(gain_hbm, gain_ref, local_sem.at[9])
    up_copy = pltpu.make_async_copy(up_hbm, up_ref, local_sem.at[10])
    target_copy = pltpu.make_async_copy(target_hbm, target_ref, local_sem.at[4])
    down_copy = pltpu.make_async_copy(down_hbm, down_ref, local_sem.at[5])

    def x_copy(i):
        at = pl.ds(pl.multiple_of(i * part, part), part)
        return pltpu.make_async_copy(x_hbm.at[at], x_ref.at[at], local_sem.at[i])

    scales_copy.start()
    outer_copy.start()
    codes_copy.start()
    gain_copy.start()
    for i in range(4):
        x_copy(i).start()
    down_copy.start()
    up_copy.start()
    target_copy.start()

    def mirror(px, j):
        return j + px * (pieces - 1 - 2 * j)

    def chunk(layer, y, c, q):
        start = (layer * 2 + y) * rows + (q * 2 + c) * high
        return weight_ref.at[pl.ds(pl.multiple_of(start, high), high)]

    def mine_slot(at, layer, q):
        return jnp.where(layer > at, layer - 1, layer) * pieces + q

    def other_slot(layer, q):
        return (layers - 1 + layer) * pieces + q

    def slot(layer, y, q):
        return jnp.where(y == cy, mine_slot(cl, layer, q), other_slot(layer, q))

    def link_copy(layer, y, q, place, send_sem, peer):
        ref = chunk(layer, y, cc, q)
        return pltpu.make_async_remote_copy(
            src_ref=ref,
            dst_ref=ref,
            send_sem=send_sem,
            recv_sem=link_recv.at[place],
            device_id=peer,
            device_id_type=MESH,
        )

    def z_copy(layer, j, step):
        sem = z_send.at[jnp.where((layer == cl) & (step > 0), layers, layer)]
        q = mirror(cx, j)
        return link_copy(layer, cy, q, mine_slot(cl + step, layer, q), sem, z_peer(step))

    def x_piece(layer, y, j):
        q = mirror(cx, j)
        return link_copy(layer, y, q, slot(layer, y, q), x_send.at[0], x_peer)

    def y_piece(layer, j):
        q = mirror(cx, j)
        return link_copy(layer, cy, q, other_slot(layer, q), y_send.at[0], y_peer)

    def core_copy(layer, y, q):
        ref = chunk(layer, y, cc, q)
        return pltpu.make_async_remote_copy(
            src_ref=ref,
            dst_ref=ref,
            send_sem=core_send.at[y],
            recv_sem=core_recv.at[(layer * 2 + y) * groups + q // group],
            device_id=sibling,
            device_id_type=MESH,
        )

    def landed(ref, sem):
        pltpu.make_async_copy(ref, ref, sem).wait()

    def arrived(layer, y, q):
        landed(chunk(layer, y, cc, q), link_recv.at[slot(layer, y, q)])

    def some_rows(count):
        return weight_ref.at[pl.ds(0, count * high)]

    deep = lax.broadcasted_iota(jnp.int32, spread_ref.shape, 0)
    wide = lax.broadcasted_iota(jnp.int32, spread_ref.shape, 1)
    spread_ref[...] = jnp.where(
        (deep % 128) * 4 + deep // 128 == wide, 1.0, 0.0
    ).astype(jnp.bfloat16)

    words = codes_ref.shape[1]
    lanes = scales_ref.shape[1]
    per_row = scales_ref.shape[0] * lanes // rows
    line = rows // scales_ref.shape[0]
    run = words // (4 * per_row)
    bunch = rows // groups
    lines = scales_ref.shape[0] // groups
    place = lax.broadcasted_iota(jnp.int32, pick_ref.shape, 0)
    word = lax.broadcasted_iota(jnp.int32, pick_ref.shape, 1)
    pick = (place % per_row == word // (4 * run)) & ((word // run) % 4 == place // lanes)
    pick_ref[...] = jnp.where(pick, 1.0, 0.0).astype(jnp.bfloat16)
    row = lax.broadcasted_iota(jnp.int32, (bunch, lanes), 0)
    lane = lax.broadcasted_iota(jnp.int32, (bunch, lanes), 1)
    mine = lane // per_row == row % line
    outer_count = outer_ref.shape[1]
    outer_rows = rows // outer_count
    outer_row = lax.broadcasted_iota(jnp.int32, (bunch, outer_count), 0) // outer_rows
    outer_lane = lax.broadcasted_iota(jnp.int32, (bunch, outer_count), 1)

    def unpack(index):
        scale_words = jnp.concatenate(
            [
                jnp.broadcast_to(scales_ref[pl.ds(index * lines + i, 1), :], (line, lanes))
                for i in range(lines)
            ],
            axis=0,
        )
        values = []
        for byte in range(4):
            value = jnp.bitwise_and(jnp.right_shift(scale_words, 8 * byte), 255)
            values.append(jnp.where(mine, value.astype(jnp.float32), 0.0).astype(jnp.bfloat16))
        code = jnp.dot(
            jnp.concatenate(values, axis=1), pick_ref[...], preferred_element_type=jnp.float32
        )
        mask = outer_row + index * (bunch // outer_rows) == outer_lane
        second = jnp.sum(
            jnp.where(mask, outer_ref[...].astype(jnp.float32), 0.0), axis=1, keepdims=True
        )
        second = jnp.exp2(second / 128.0 - 6.0)
        at = pl.ds(pl.multiple_of(index * bunch, bunch), bunch)
        scale_ref[at, :] = (code + 0.5) / 256.0 * second

    def decode(c, index):
        starts = [
            pl.multiple_of(((index * group + i) * 2 + c) * high, high) for i in range(group)
        ]
        for h in range(words // 128):
            span = pl.ds(h * 128, 128)
            code_words = jnp.concatenate([codes_ref[pl.ds(s, high), span] for s in starts])
            scale = jnp.concatenate([scale_ref[pl.ds(s, high), span] for s in starts])
            planes = [
                (nibble_levels(code_words, plane) * scale).astype(jnp.bfloat16)
                for plane in range(4)
            ]
            ordered = jnp.dot(
                jnp.concatenate(planes, axis=1),
                spread_ref[...],
                preferred_element_type=jnp.float32,
            ).astype(jnp.bfloat16)
            for i, s in enumerate(starts):
                weight_ref[
                    pl.ds(pl.multiple_of(f * rows + s, high), high), pl.ds(h * 512, 512)
                ] = ordered[i * high : (i + 1) * high]

    def turned(index):
        return index + cx * (groups - 1 - 2 * index)

    def own_sends(index):
        for i in range(group):
            j = index * group + i
            for step in (-1, 1):

                @pl.when(inside(cl + step) & (j < by_z))
                def _():
                    z_copy(cl, j, step).start()

            pl.when(j < early)(lambda: y_piece(cl, j).start())

    scales_copy.wait()
    outer_copy.wait()
    unpack(turned(0))
    codes_copy.wait()
    decode(cc, turned(0))
    neighbours = 3 + jnp.where(cl > 0, 1, 0) + jnp.where(cl < layers - 1, 1, 0)
    pl.semaphore_wait(barrier, neighbours)
    own_sends(0)

    def rest(index, carry):
        unpack(turned(index))
        decode(cc, turned(index))
        own_sends(index)
        return carry

    lax.fori_loop(1, groups, rest, 0)
    gain_copy.wait()
    wide_gain_ref[...] = gain_ref[...].astype(jnp.float32)

    tile = min(1024, width)

    def normalize(i):
        pl.when(i % (blocks // 4) == 0)(lambda: x_copy(i // (blocks // 4)).wait())
        at = pl.ds(pl.multiple_of(i * block, block), block)
        total = jnp.zeros((block, 128), jnp.float32)
        for t in range(width // tile):
            v = x_ref[at, pl.ds(t * tile, tile)].astype(jnp.float32)
            v = v * v
            for k in range(tile // 128):
                total += v[:, k * 128 : (k + 1) * 128]
        inverse = lax.rsqrt(jnp.sum(total, axis=1, keepdims=True) / width + epsilon)
        for t in range(width // 128):
            span = pl.ds(t * 128, 128)
            v = x_ref[at, span].astype(jnp.float32)
            x_ref[at, span] = (v * inverse * wide_gain_ref[pl.ds(t, 1), :]).astype(jnp.bfloat16)

    def adapter(step):
        at = pl.ds(pl.multiple_of(step * (width // 8), width // 8), width // 8)
        partial = lax.dot_general(
            x_ref[:, at],
            down_ref[:, at],
            (((1,), (1,)), ((), ())),
            preferred_element_type=jnp.float32,
        )

        @pl.when(step == 0)
        def _():
            low_ref[...] = partial

        @pl.when(step > 0)
        def _():
            low_ref[...] += partial

    def adapter_up():
        up_copy.wait()

        acc_ref[...] += adapter_scale * jnp.dot(
            low_ref[...].astype(jnp.bfloat16), up_ref[...], preferred_element_type=jnp.float32
        )

    def whole(layer, y, index, is_own):
        @pl.when(jnp.logical_not(is_own))
        def _():
            landed(some_rows(group), core_recv.at[(layer * 2 + y) * groups + index])

    def product(layer, y, index):
        size = rows // groups
        at = pl.ds(pl.multiple_of((layer * 2 + y) * rows + index * size, size), size)
        return jnp.dot(x_ref[:, at], weight_ref[at, :], preferred_element_type=jnp.float32)

    def multiply(layer, y, index, is_own):
        whole(layer, y, index, is_own)
        acc_ref[...] += product(layer, y, index)

    shorter = jnp.minimum(cl, layers - 1 - cl)
    longer = jnp.where(cl * 2 < layers - 1, 1, -1)

    def hops_of(v):
        return jnp.where(v <= 2 * shorter, (v + 1) // 2, v - shorter)

    def layer_of(v):
        near = v <= 2 * shorter
        away = hops_of(v)
        side = jnp.where(near & (v % 2 == 0), -longer, longer)
        return jnp.clip(cl + side * away, 0, layers - 1)

    def stage(k):
        k = jnp.maximum(k, 0)
        return lax.div(k, by_z) + 1, lax.rem(k, by_z)

    def z_stage(k):
        s, j = stage(k)
        past = k - turn
        s = jnp.where(past >= 0, layers - 1, s)
        j = jnp.where(past >= 0, past, j)
        second = (past >= by_y) & (past < by_z)
        s = jnp.where(second, layers - 2, s)
        j = jnp.where(past >= by_z, past - by_z + by_y, j)
        return s, j

    def send_stage(k):
        v, j = stage(k)
        past = k - turn
        return jnp.where(past >= 0, layers - 1, v), jnp.where(past >= 0, past, j)

    def held(hop, j):
        return (hop == layers - 3) & (j >= by_y)

    def z_event(k):
        s, j = z_stage(k)
        q = mirror(cx, j)
        late = k - (layers - 3) * by_z
        for step in (-1, 1):
            layer = cl + step * s

            @pl.when(inside(layer))
            def _():
                arrived(layer, cy, q)
                go = inside(cl - step) & jnp.logical_not(held(s, j))
                pl.when(go)(lambda: z_copy(layer, j, -step).start())
                core_copy(layer, cy, q).start()

            if layers > 3:
                layer_held = cl + step * (layers - 3)
                waiting = (late >= by_y) & (late < by_z)

                @pl.when(waiting & inside(layer_held) & inside(cl - step))
                def _():
                    z_copy(layer_held, late, -step).start()

    def own_index(v, j):
        v = jnp.minimum(v, layers - 2)
        return early + (v - 1) * spare + j - by_y

    def send_event(k):
        v, j = send_stage(k)
        layer = layer_of(v)
        pl.when((v < layers - 1) & (j < pieces - by_z))(
            lambda: x_piece(layer, cy, j).start()
        )
        pl.when(j < by_y)(lambda: y_piece(layer, j).start())
        o = own_index(v, j)
        pl.when((j >= by_y) & (o < own_y))(lambda: y_piece(cl, o).start())

    def y_event(k):
        v, j = send_stage(k)
        o = jnp.where(k < 0, k + early, own_index(v, j))
        moving = (k >= 0) & (j < by_y)
        layer = jnp.where(moving, layer_of(v), cl)
        i = jnp.where(moving, j, o)

        @pl.when(moving | (o < own_y))
        def _():
            q = mirror(cx, i)
            arrived(layer, 1 - cy, q)
            pl.when(moving | (o < pieces - own_y))(
                lambda: x_piece(layer, 1 - cy, i).start()
            )
            core_copy(layer, 1 - cy, q).start()

    def x_event(k):
        v, j = send_stage(k)
        moving = (k >= 0) & (j < by_y)
        o = k + early
        layer = jnp.where(k < 0, cl, layer_of(v))
        i = jnp.where(k < 0, o, j)
        q = mirror(1 - cx, i)

        @pl.when((k >= 0) & (v < layers - 1) & (j < pieces - by_z))
        def _():
            arrived(layer, cy, q)
            core_copy(layer, cy, q).start()

        @pl.when(moving | ((k < 0) & (o < pieces - own_y)))
        def _():
            arrived(layer, 1 - cy, q)
            core_copy(layer, 1 - cy, q).start()

    def last_x_event(k):
        v = layers - 1
        layer = layer_of(v)
        count = pieces - by_z
        j = k - p["last_x"]
        pl.when((j >= 0) & (j < count))(lambda: x_piece(layer, cy, j).start())
        i = j - p["x_lag"]

        @pl.when((i >= 0) & (i < count))
        def _():
            q = mirror(1 - cx, i)
            arrived(layer, cy, q)
            core_copy(layer, cy, q).start()

    each = p["each"]
    often = max(1, (p["normal"] - 1) // groups)

    def early_work(k):
        def some(i, carry):
            normalize(i)
            return carry

        lax.fori_loop(jnp.minimum(k * each, blocks), jnp.minimum((k + 1) * each, blocks), some, 0)
        pl.when((lax.rem(k, often) == 0) & (k < groups * often))(
            lambda: decode(1 - cc, lax.div(k, often))
        )

        @pl.when(k == p["normal"] - 1)
        def _():
            acc_ref[...] = jnp.zeros(acc_ref.shape, jnp.float32)
            down_copy.wait()

    def extra_of(kind):
        layer = layer_of(layers - 1 - lax.div(jnp.maximum(kind - 2, 0), 2))
        layer = jnp.where(kind < 2, cl, layer)
        y = jnp.where(lax.rem(kind, 2) == 0, cy, 1 - cy)
        return layer, y

    def extra_work(k):
        for order in (1, 2):
            chosen = [e for e in p["extras"] if e[1] == order]

            @pl.when(k >= min([e[0] for e in chosen], default=p["total"]))
            def _():
                choice = jnp.int32(-1)
                for when, _, a, b in chosen:
                    choice = jnp.where(k == when, a * groups + b, choice)

                @pl.when(choice >= 0)
                def _():
                    kind, index = lax.div(choice, groups), lax.rem(choice, groups)
                    layer, y = extra_of(kind)
                    multiply(layer, y, turned(index), kind == 0)

    def late_work(k):
        past = k - ready
        v, j = stage(past)
        for i in range(p["per"]):
            index = j * p["per"] + i

            @pl.when((v < layers - 2) & (index < 2 * groups))
            def _():
                y = jnp.where(index < groups, cy, 1 - cy)
                multiply(layer_of(v), y, turned(lax.rem(index, groups)), False)

        pl.when(past < 8)(lambda: adapter(past))
        pl.when(past == 8)(adapter_up)

    def one_slot(k, carry):
        @pl.when(k < slots)
        def _():
            z_event(k)
            send_event(k)

        pl.when(k >= y_lag - early)(lambda: y_event(k - y_lag))
        pl.when(k >= lag - early)(lambda: x_event(k - lag))
        pl.when(k >= p["last_x"])(lambda: last_x_event(k))
        pl.when(k < p["normal"])(lambda: early_work(k))
        pl.when(k >= ready)(lambda: late_work(k))
        extra_work(k)
        return carry

    lax.fori_loop(0, p["total"], one_slot, 0)
    target_copy.wait()
    for kind, index in p["tail"][:-1]:
        layer, y = extra_of(jnp.int32(kind))
        multiply(layer, y, turned(index), kind == 0)
    kind, index = p["tail"][-1]
    layer, y = extra_of(jnp.int32(kind))
    whole(layer, y, turned(index), kind == 0)
    exact = acc_ref[...] + product(layer, y, turned(index))
    out_ref[...] = exact.astype(jnp.bfloat16)
    error = exact - target_ref[...].astype(jnp.float32)
    error = error * error
    total = jnp.zeros((tokens, 128), jnp.float32)
    for k in range(columns // 128):
        total += error[:, k * 128 : (k + 1) * 128]
    share = jnp.zeros((8, 128), jnp.float32)
    for k in range(tokens // 8):
        share += total[k * 8 : (k + 1) * 8]

    fsdp = layers * 2
    members = 4 * fsdp
    spot = g * fsdp + f
    losses_ref[spot] = jnp.sum(share, axis=0, keepdims=True)

    def tell(j, carry):
        to = f + j
        to = jnp.where(to >= fsdp, to - fsdp, to)
        for i in range(4):

            @pl.when((i > 0) | (j > 0))
            def _():
                pltpu.make_async_remote_copy(
                    src_ref=losses_ref.at[spot],
                    dst_ref=losses_ref.at[spot],
                    send_sem=loss_sem.at[0],
                    recv_sem=loss_sem.at[1],
                    device_id=((g + i) % 4, to),
                    device_id_type=MESH,
                ).start()

        return carry

    lax.fori_loop(0, fsdp, tell, 0)

    def sent(layer, carry):
        up = inside(cl + 1) & (layer <= cl)
        down = inside(cl - 1) & (layer >= cl)
        own_up = up & (layer == cl)
        pl.when(own_up)(lambda: landed(some_rows(by_z), z_send.at[layers]))
        pl.when(down | (up & (layer != cl)))(
            lambda: landed(some_rows(by_z), z_send.at[layer])
        )
        return carry

    lax.fori_loop(0, layers, sent, 0)
    away = layers - 1
    landed(some_rows(away * by_y + own_y), y_send.at[0])
    landed(some_rows(away * (by_y + pieces - by_z) + pieces - own_y), x_send.at[0])
    landed(some_rows(away * pieces), core_send.at[cy])
    landed(some_rows(layers * pieces), core_send.at[1 - cy])
    others = losses_ref.at[pl.ds(0, members - 1)]
    landed(others, loss_sem.at[1])
    everyone = jnp.sum(losses_ref[...], axis=0)
    loss_ref[...] = jnp.sum(everyone, axis=1, keepdims=True) / (tokens * fsdp * columns)
    landed(others, loss_sem.at[0])


def per_device(fsdp, x, gain, codes, scales, outer, down, up, target):
    tokens, width = x.shape
    columns = up.shape[1]
    rows = codes.shape[0]
    layers = fsdp // 2
    pieces = rows // 2 // max(16, rows // 32)
    groups = min(4, rows // 128)
    hbm = pl.BlockSpec(memory_space=pltpu.HBM)
    dma = pltpu.SemaphoreType.DMA
    gain = gain.reshape(-1, 128)
    outer = outer.reshape(1, -1)
    operands = (x, gain, codes, scales, outer, down.T, up, target)
    operands = [pltpu.with_memory_space_constraint(a, pltpu.HBM) for a in operands]
    kv, loss = pl.pallas_call(
        functools.partial(kernel, layers, pieces, groups),
        out_shape=(
            pltpu.VMEM((tokens, columns), jnp.bfloat16),
            pltpu.VMEM((1, 1), jnp.float32),
        ),
        in_specs=[hbm] * 8,
        out_specs=(
            pl.BlockSpec(memory_space=pltpu.VMEM),
            pl.BlockSpec(memory_space=pltpu.VMEM),
        ),
        scratch_shapes=[
            pltpu.VMEM((tokens, width), jnp.bfloat16),
            pltpu.VMEM((width, columns), jnp.bfloat16),
            pltpu.VMEM((tokens, columns), jnp.float32),
            pltpu.VMEM((tokens, columns), jnp.bfloat16),
            pltpu.VMEM(down.shape[::-1], jnp.bfloat16),
            pltpu.VMEM(up.shape, jnp.bfloat16),
            pltpu.VMEM(gain.shape, jnp.bfloat16),
            pltpu.VMEM(codes.shape, jnp.int32),
            pltpu.VMEM(scales.shape, jnp.int32),
            pltpu.VMEM(outer.shape, jnp.int32),
            pltpu.VMEM((512, 512), jnp.bfloat16),
            pltpu.VMEM((4 * scales.shape[1], codes.shape[1]), jnp.bfloat16),
            pltpu.VMEM(codes.shape, jnp.float32),
            pltpu.VMEM((width // 128, 128), jnp.float32),
            pltpu.VMEM((tokens, down.shape[1]), jnp.float32),
            pltpu.VMEM((4 * fsdp, 1, 128), jnp.float32),
            dma((11,)),
            dma((layers + 1,)),
            dma((1,)),
            dma((1,)),
            dma((2,)),
            dma(((layers * 2 - 1) * pieces,)),
            dma((layers * 2 * groups,)),
            dma((2,)),
        ],
        compiler_params=pltpu.CompilerParams(
            collective_id=0, has_side_effects=True, vmem_limit_bytes=40 * 1024 * 1024
        ),
    )(*operands)
    return kv, loss.reshape(())


def solution(mesh):
    placed = (
        P(("grp", "fsdp"), None),
        P(),
        P("fsdp", None),
        P("fsdp", None),
        P("fsdp"),
        P(),
        P(),
        P(("grp", "fsdp"), None),
    )
    return jax.shard_map(
        functools.partial(per_device, mesh.shape["fsdp"]),
        mesh=mesh,
        in_specs=placed,
        out_specs=(P(("grp", "fsdp"), None), P()),
        check_vma=False,
    )
```

```python
import functools

import jax
import jax.numpy as jnp
from jax import lax
from jax.experimental import pallas as pl
from jax.experimental.pallas import tpu as pltpu
from jax.sharding import PartitionSpec as P

adapter_scale = 0.25
epsilon = 1e-06
nf4_levels = (
    -1.0,
    -0.6961928009986877,
    -0.5250730514526367,
    -0.39491748809814453,
    -0.28444138169288635,
    -0.18477343022823334,
    -0.09105003625154495,
    0.0,
    0.07958029955625534,
    0.16093020141124725,
    0.24611230194568634,
    0.33791524171066284,
    0.44070982933044434,
    0.5626170039176941,
    0.7229568362236023,
    1.0,
)
MESH = pl.DeviceIdType.MESH
OWN, EARLY, YLAG, XLAG = 14, 4, 4, 3


def nibble_levels(words, plane):
    values = [jnp.float32(level) for level in nf4_levels]
    for bit in range(4):
        is_set = jnp.bitwise_and(words, 1 << (4 * plane + bit)) != 0
        values = [
            jnp.where(is_set, values[2 * i + 1], values[2 * i])
            for i in range(len(values) // 2)
        ]
    return values[0]


def plan(layers, pieces, groups, blocks):
    by_z = max(pieces // 2, pieces * 13 // 16)
    by_y = pieces // 2
    own_y = pieces * OWN // 16
    early = min(EARLY, own_y)
    y_lag, x_lag = YLAG, XLAG
    lag = y_lag + x_lag
    group = pieces // groups
    spare = by_z - by_y
    turn = (layers - 3) * by_z + by_y
    slots = turn + by_z + by_z - by_y
    ready = max(by_z, by_y + lag)
    per = -(-2 * groups // by_z)
    each = -(-blocks // (ready - 1))
    normal = -(-blocks // each)

    def own_slot(o):
        if o < early:
            return o - early
        o -= early
        if o < (layers - 3) * spare:
            return o // spare * by_z + by_y + o % spare
        return turn + by_y + o - (layers - 3) * spare

    def z_slot(hop, i):
        if hop == layers - 1:
            return turn + i if i < by_y else turn + by_z + i - by_y
        if hop == layers - 2:
            return (layers - 3) * by_z + i if i < by_y else turn + i
        return (hop - 1) * by_z + i

    def send_slot(v, i):
        return turn + i if v == layers - 1 else (v - 1) * by_z + i

    last_x = turn + by_y + y_lag
    total = max(slots, last_x + x_lag + pieces - by_z, own_slot(own_y - 1) + y_lag + 1)
    total = max(total, (layers - 4) * by_z + ready + -(-2 * groups // per))

    def seen(kind, i):
        twin = pieces - 1 - i
        if kind == 0:
            return normal - 1
        if kind == 1:
            return own_slot(i) + y_lag if i < own_y else own_slot(twin) + lag
        v = layers - 1 - (kind - 2) // 2
        if kind % 2 == 0:
            when = 0
            for shorter in range((layers + 1) // 2):
                hop = (v + 1) // 2 if v <= 2 * shorter else v - shorter
                over = last_x + x_lag + twin if v == layers - 1 else send_slot(v, twin) + lag
                when = max(when, z_slot(hop, i) if i < by_z else over)
            return when
        return send_slot(v, i) + y_lag if i < by_y else send_slot(v, twin) + lag

    items = []
    for kind in range(6):
        for g in range(groups):
            when = max(seen(kind, i) for i in range(g * group, (g + 1) * group))
            when += 1 if when >= slots - 4 else 2
            items.append((max(when, normal), kind, g))
    items.sort()
    extras, tail = [], []
    taken = {}
    for when, kind, g in items:
        slot = when
        while ready <= slot < ready + 9 or taken.get(slot, 0) >= (1 if slot < turn + by_y else 2):
            slot += 1
        taken[slot] = taken.get(slot, 0) + 1
        if slot < slots - 1:
            extras.append((slot, taken[slot], kind, g))
        else:
            tail.append((kind, g))
    return dict(
        by_z=by_z,
        by_y=by_y,
        own_y=own_y,
        early=early,
        y_lag=y_lag,
        lag=lag,
        group=group,
        turn=turn,
        last_x=last_x,
        x_lag=x_lag,
        slots=slots,
        spare=spare,
        ready=ready,
        per=per,
        each=each,
        normal=normal,
        total=total,
        extras=extras,
        tail=tail,
    )


def kernel(
    layers,
    pieces,
    groups,
    x_hbm,
    gain_hbm,
    codes_hbm,
    scales_hbm,
    outer_hbm,
    down_hbm,
    up_hbm,
    target_hbm,
    out_ref,
    loss_ref,
    x_ref,
    weight_ref,
    acc_ref,
    target_ref,
    down_ref,
    up_ref,
    gain_ref,
    codes_ref,
    scales_ref,
    outer_ref,
    spread_ref,
    pick_ref,
    scale_ref,
    wide_gain_ref,
    low_ref,
    losses_ref,
    local_sem,
    z_send,
    x_send,
    y_send,
    core_send,
    link_recv,
    core_recv,
    loss_sem,
):
    g = lax.axis_index("grp")
    f = lax.axis_index("fsdp")
    cx, cc = g // 2, g % 2
    cl, cy = f // 2, f % 2
    tokens, width = x_ref.shape
    columns = acc_ref.shape[1]
    rows = codes_ref.shape[0]
    high = rows // 2 // pieces
    block = min(16, tokens // 4)
    blocks = tokens // block
    p = plan(layers, pieces, groups, blocks)
    by_z, by_y, own_y, early = p["by_z"], p["by_y"], p["own_y"], p["early"]
    y_lag, lag, group, spare = p["y_lag"], p["lag"], p["group"], p["spare"]
    slots, ready, turn = p["slots"], p["ready"], p["turn"]

    sibling = (cx * 2 + 1 - cc, f)
    x_peer = ((1 - cx) * 2 + cc, f)
    y_peer = (g, cl * 2 + 1 - cy)

    def z_peer(step):
        return (g, (cl + step) * 2 + cy)

    def inside(layer):
        return (layer >= 0) & (layer < layers)

    barrier = pltpu.get_barrier_semaphore()
    for peer in (x_peer, y_peer, sibling):
        pl.semaphore_signal(barrier, inc=1, device_id=peer, device_id_type=MESH)
    for step in (-1, 1):

        @pl.when(inside(cl + step))
        def _():
            pl.semaphore_signal(barrier, inc=1, device_id=z_peer(step), device_id_type=MESH)

    part = tokens // 4
    scales_copy = pltpu.make_async_copy(scales_hbm, scales_ref, local_sem.at[6])
    outer_copy = pltpu.make_async_copy(outer_hbm, outer_ref, local_sem.at[7])

    def codes_copy(index, place):
        bunch = rows // groups
        start = (index + cx * (groups - 1 - 2 * index)) * bunch
        at = pl.ds(pl.multiple_of(start, bunch), bunch)
        return pltpu.make_async_copy(codes_hbm.at[at], codes_ref.at[at], local_sem.at[place])

    gain_copy = pltpu.make_async_copy(gain_hbm, gain_ref, local_sem.at[9])
    up_copy = pltpu.make_async_copy(up_hbm, up_ref, local_sem.at[10])
    target_copy = pltpu.make_async_copy(target_hbm, target_ref, local_sem.at[4])
    down_copy = pltpu.make_async_copy(down_hbm, down_ref, local_sem.at[5])

    def x_copy(i):
        at = pl.ds(pl.multiple_of(i * part, part), part)
        return pltpu.make_async_copy(x_hbm.at[at], x_ref.at[at], local_sem.at[i])

    scales_copy.start()
    outer_copy.start()
    codes_copy(0, 8).start()
    for i in range(1, groups):
        codes_copy(i, 10 + i).start()
    gain_copy.start()
    for i in range(4):
        x_copy(i).start()
    down_copy.start()
    up_copy.start()
    target_copy.start()

    def mirror(px, j):
        return j + px * (pieces - 1 - 2 * j)

    def chunk(layer, y, c, q):
        start = (layer * 2 + y) * rows + (q * 2 + c) * high
        return weight_ref.at[pl.ds(pl.multiple_of(start, high), high)]

    def mine_slot(at, layer, q):
        return jnp.where(layer > at, layer - 1, layer) * pieces + q

    def other_slot(layer, q):
        return (layers - 1 + layer) * pieces + q

    def slot(layer, y, q):
        return jnp.where(y == cy, mine_slot(cl, layer, q), other_slot(layer, q))

    def link_copy(layer, y, q, place, send_sem, peer):
        ref = chunk(layer, y, cc, q)
        return pltpu.make_async_remote_copy(
            src_ref=ref,
            dst_ref=ref,
            send_sem=send_sem,
            recv_sem=link_recv.at[place],
            device_id=peer,
            device_id_type=MESH,
        )

    def z_copy(layer, j, step):
        sem = z_send.at[jnp.where((layer == cl) & (step > 0), layers, layer)]
        q = mirror(cx, j)
        return link_copy(layer, cy, q, mine_slot(cl + step, layer, q), sem, z_peer(step))

    def x_piece(layer, y, j):
        q = mirror(cx, j)
        return link_copy(layer, y, q, slot(layer, y, q), x_send.at[0], x_peer)

    def y_piece(layer, j):
        q = mirror(cx, j)
        return link_copy(layer, cy, q, other_slot(layer, q), y_send.at[0], y_peer)

    def core_copy(layer, y, q):
        ref = chunk(layer, y, cc, q)
        return pltpu.make_async_remote_copy(
            src_ref=ref,
            dst_ref=ref,
            send_sem=core_send.at[y],
            recv_sem=core_recv.at[(layer * 2 + y) * groups + q // group],
            device_id=sibling,
            device_id_type=MESH,
        )

    def landed(ref, sem):
        pltpu.make_async_copy(ref, ref, sem).wait()

    def arrived(layer, y, q):
        landed(chunk(layer, y, cc, q), link_recv.at[slot(layer, y, q)])

    def some_rows(count):
        return weight_ref.at[pl.ds(0, count * high)]

    deep = lax.broadcasted_iota(jnp.int32, spread_ref.shape, 0)
    wide = lax.broadcasted_iota(jnp.int32, spread_ref.shape, 1)
    spread_ref[...] = jnp.where(
        (deep % 128) * 4 + deep // 128 == wide, 1.0, 0.0
    ).astype(jnp.bfloat16)

    words = codes_ref.shape[1]
    lanes = scales_ref.shape[1]
    per_row = scales_ref.shape[0] * lanes // rows
    line = rows // scales_ref.shape[0]
    run = words // (4 * per_row)
    bunch = rows // groups
    lines = scales_ref.shape[0] // groups
    place = lax.broadcasted_iota(jnp.int32, pick_ref.shape, 0)
    word = lax.broadcasted_iota(jnp.int32, pick_ref.shape, 1)
    pick = (place % per_row == word // (4 * run)) & ((word // run) % 4 == place // lanes)
    pick_ref[...] = jnp.where(pick, 1.0, 0.0).astype(jnp.bfloat16)
    row = lax.broadcasted_iota(jnp.int32, (bunch, lanes), 0)
    lane = lax.broadcasted_iota(jnp.int32, (bunch, lanes), 1)
    mine = lane // per_row == row % line
    outer_count = outer_ref.shape[1]
    outer_rows = rows // outer_count
    outer_row = lax.broadcasted_iota(jnp.int32, (bunch, outer_count), 0) // outer_rows
    outer_lane = lax.broadcasted_iota(jnp.int32, (bunch, outer_count), 1)

    def unpack(index):
        scale_words = jnp.concatenate(
            [
                jnp.broadcast_to(scales_ref[pl.ds(index * lines + i, 1), :], (line, lanes))
                for i in range(lines)
            ],
            axis=0,
        )
        values = []
        for byte in range(4):
            value = jnp.bitwise_and(jnp.right_shift(scale_words, 8 * byte), 255)
            values.append(jnp.where(mine, value.astype(jnp.float32), 0.0).astype(jnp.bfloat16))
        code = jnp.dot(
            jnp.concatenate(values, axis=1), pick_ref[...], preferred_element_type=jnp.float32
        )
        mask = outer_row + index * (bunch // outer_rows) == outer_lane
        second = jnp.sum(
            jnp.where(mask, outer_ref[...].astype(jnp.float32), 0.0), axis=1, keepdims=True
        )
        second = jnp.exp2(second / 128.0 - 6.0)
        at = pl.ds(pl.multiple_of(index * bunch, bunch), bunch)
        scale_ref[at, :] = (code + 0.5) / 256.0 * second

    def decode(c, index):
        starts = [
            pl.multiple_of(((index * group + i) * 2 + c) * high, high) for i in range(group)
        ]
        for h in range(words // 128):
            span = pl.ds(h * 128, 128)
            code_words = jnp.concatenate([codes_ref[pl.ds(s, high), span] for s in starts])
            scale = jnp.concatenate([scale_ref[pl.ds(s, high), span] for s in starts])
            planes = [
                (nibble_levels(code_words, plane) * scale).astype(jnp.bfloat16)
                for plane in range(4)
            ]
            ordered = jnp.dot(
                jnp.concatenate(planes, axis=1),
                spread_ref[...],
                preferred_element_type=jnp.float32,
            ).astype(jnp.bfloat16)
            for i, s in enumerate(starts):
                weight_ref[
                    pl.ds(pl.multiple_of(f * rows + s, high), high), pl.ds(h * 512, 512)
                ] = ordered[i * high : (i + 1) * high]

    def turned(index):
        return index + cx * (groups - 1 - 2 * index)

    def own_sends(index):
        for i in range(group):
            j = index * group + i
            for step in (-1, 1):

                @pl.when(inside(cl + step) & (j < by_z))
                def _():
                    z_copy(cl, j, step).start()

            pl.when(j < early)(lambda: y_piece(cl, j).start())

    scales_copy.wait()
    outer_copy.wait()
    unpack(turned(0))
    codes_copy(0, 8).wait()
    decode(cc, turned(0))
    neighbours = 3 + jnp.where(cl > 0, 1, 0) + jnp.where(cl < layers - 1, 1, 0)
    pl.semaphore_wait(barrier, neighbours)
    own_sends(0)

    def rest(index, carry):
        unpack(turned(index))
        codes_copy(index, 10 + index).wait()
        decode(cc, turned(index))
        own_sends(index)
        return carry

    lax.fori_loop(1, groups, rest, 0)
    gain_copy.wait()
    wide_gain_ref[...] = gain_ref[...].astype(jnp.float32)

    tile = min(1024, width)

    def normalize(i):
        pl.when(i % (blocks // 4) == 0)(lambda: x_copy(i // (blocks // 4)).wait())
        at = pl.ds(pl.multiple_of(i * block, block), block)
        total = jnp.zeros((block, 128), jnp.float32)
        for t in range(width // tile):
            v = x_ref[at, pl.ds(t * tile, tile)].astype(jnp.float32)
            v = v * v
            for k in range(tile // 128):
                total += v[:, k * 128 : (k + 1) * 128]
        inverse = lax.rsqrt(jnp.sum(total, axis=1, keepdims=True) / width + epsilon)
        for t in range(width // 128):
            span = pl.ds(t * 128, 128)
            v = x_ref[at, span].astype(jnp.float32)
            x_ref[at, span] = (v * inverse * wide_gain_ref[pl.ds(t, 1), :]).astype(jnp.bfloat16)

    def adapter(step):
        at = pl.ds(pl.multiple_of(step * (width // 8), width // 8), width // 8)
        partial = lax.dot_general(
            x_ref[:, at],
            down_ref[:, at],
            (((1,), (1,)), ((), ())),
            preferred_element_type=jnp.float32,
        )

        @pl.when(step == 0)
        def _():
            low_ref[...] = partial

        @pl.when(step > 0)
        def _():
            low_ref[...] += partial

    def adapter_up():
        up_copy.wait()

        acc_ref[...] += adapter_scale * jnp.dot(
            low_ref[...].astype(jnp.bfloat16), up_ref[...], preferred_element_type=jnp.float32
        )

    def whole(layer, y, index, is_own):
        @pl.when(jnp.logical_not(is_own))
        def _():
            landed(some_rows(group), core_recv.at[(layer * 2 + y) * groups + index])

    def product(layer, y, index):
        size = rows // groups
        at = pl.ds(pl.multiple_of((layer * 2 + y) * rows + index * size, size), size)
        return jnp.dot(x_ref[:, at], weight_ref[at, :], preferred_element_type=jnp.float32)

    def multiply(layer, y, index, is_own):
        whole(layer, y, index, is_own)
        acc_ref[...] += product(layer, y, index)

    shorter = jnp.minimum(cl, layers - 1 - cl)
    longer = jnp.where(cl * 2 < layers - 1, 1, -1)

    def hops_of(v):
        return jnp.where(v <= 2 * shorter, (v + 1) // 2, v - shorter)

    def layer_of(v):
        near = v <= 2 * shorter
        away = hops_of(v)
        side = jnp.where(near & (v % 2 == 0), -longer, longer)
        return jnp.clip(cl + side * away, 0, layers - 1)

    def stage(k):
        k = jnp.maximum(k, 0)
        return lax.div(k, by_z) + 1, lax.rem(k, by_z)

    def z_stage(k):
        s, j = stage(k)
        past = k - turn
        s = jnp.where(past >= 0, layers - 1, s)
        j = jnp.where(past >= 0, past, j)
        second = (past >= by_y) & (past < by_z)
        s = jnp.where(second, layers - 2, s)
        j = jnp.where(past >= by_z, past - by_z + by_y, j)
        return s, j

    def send_stage(k):
        v, j = stage(k)
        past = k - turn
        return jnp.where(past >= 0, layers - 1, v), jnp.where(past >= 0, past, j)

    def held(hop, j):
        return (hop == layers - 3) & (j >= by_y)

    def z_event(k):
        s, j = z_stage(k)
        q = mirror(cx, j)
        late = k - (layers - 3) * by_z
        for step in (-1, 1):
            layer = cl + step * s

            @pl.when(inside(layer))
            def _():
                arrived(layer, cy, q)
                go = inside(cl - step) & jnp.logical_not(held(s, j))
                pl.when(go)(lambda: z_copy(layer, j, -step).start())
                core_copy(layer, cy, q).start()

            if layers > 3:
                layer_held = cl + step * (layers - 3)
                waiting = (late >= by_y) & (late < by_z)

                @pl.when(waiting & inside(layer_held) & inside(cl - step))
                def _():
                    z_copy(layer_held, late, -step).start()

    def own_index(v, j):
        v = jnp.minimum(v, layers - 2)
        return early + (v - 1) * spare + j - by_y

    def send_event(k):
        v, j = send_stage(k)
        layer = layer_of(v)
        pl.when((v < layers - 1) & (j < pieces - by_z))(
            lambda: x_piece(layer, cy, j).start()
        )
        pl.when(j < by_y)(lambda: y_piece(layer, j).start())
        o = own_index(v, j)
        pl.when((j >= by_y) & (o < own_y))(lambda: y_piece(cl, o).start())

    def y_event(k):
        v, j = send_stage(k)
        o = jnp.where(k < 0, k + early, own_index(v, j))
        moving = (k >= 0) & (j < by_y)
        layer = jnp.where(moving, layer_of(v), cl)
        i = jnp.where(moving, j, o)

        @pl.when(moving | (o < own_y))
        def _():
            q = mirror(cx, i)
            arrived(layer, 1 - cy, q)
            pl.when(moving | (o < pieces - own_y))(
                lambda: x_piece(layer, 1 - cy, i).start()
            )
            core_copy(layer, 1 - cy, q).start()

    def x_event(k):
        v, j = send_stage(k)
        moving = (k >= 0) & (j < by_y)
        o = k + early
        layer = jnp.where(k < 0, cl, layer_of(v))
        i = jnp.where(k < 0, o, j)
        q = mirror(1 - cx, i)

        @pl.when((k >= 0) & (v < layers - 1) & (j < pieces - by_z))
        def _():
            arrived(layer, cy, q)
            core_copy(layer, cy, q).start()

        @pl.when(moving | ((k < 0) & (o < pieces - own_y)))
        def _():
            arrived(layer, 1 - cy, q)
            core_copy(layer, 1 - cy, q).start()

    def last_x_event(k):
        v = layers - 1
        layer = layer_of(v)
        count = pieces - by_z
        j = k - p["last_x"]
        pl.when((j >= 0) & (j < count))(lambda: x_piece(layer, cy, j).start())
        i = j - p["x_lag"]

        @pl.when((i >= 0) & (i < count))
        def _():
            q = mirror(1 - cx, i)
            arrived(layer, cy, q)
            core_copy(layer, cy, q).start()

    each = p["each"]
    often = max(1, (p["normal"] - 1) // groups)

    def early_work(k):
        def some(i, carry):
            normalize(i)
            return carry

        lax.fori_loop(jnp.minimum(k * each, blocks), jnp.minimum((k + 1) * each, blocks), some, 0)
        pl.when((lax.rem(k, often) == 0) & (k < groups * often))(
            lambda: decode(1 - cc, lax.div(k, often))
        )

        @pl.when(k == p["normal"] - 1)
        def _():
            acc_ref[...] = jnp.zeros(acc_ref.shape, jnp.float32)
            down_copy.wait()

    def extra_of(kind):
        layer = layer_of(layers - 1 - lax.div(jnp.maximum(kind - 2, 0), 2))
        layer = jnp.where(kind < 2, cl, layer)
        y = jnp.where(lax.rem(kind, 2) == 0, cy, 1 - cy)
        return layer, y

    def extra_work(k):
        for order in (1, 2):
            chosen = [e for e in p["extras"] if e[1] == order]

            @pl.when(k >= min([e[0] for e in chosen], default=p["total"]))
            def _():
                choice = jnp.int32(-1)
                for when, _, a, b in chosen:
                    choice = jnp.where(k == when, a * groups + b, choice)

                @pl.when(choice >= 0)
                def _():
                    kind, index = lax.div(choice, groups), lax.rem(choice, groups)
                    layer, y = extra_of(kind)
                    multiply(layer, y, turned(index), kind == 0)

    def late_work(k):
        past = k - ready
        v, j = stage(past)
        for i in range(p["per"]):
            index = j * p["per"] + i

            @pl.when((v < layers - 2) & (index < 2 * groups))
            def _():
                y = jnp.where(index < groups, cy, 1 - cy)
                multiply(layer_of(v), y, turned(lax.rem(index, groups)), False)

        pl.when(past < 8)(lambda: adapter(past))
        pl.when(past == 8)(adapter_up)

    def one_slot(k, carry):
        @pl.when(k < slots)
        def _():
            z_event(k)
            send_event(k)

        pl.when(k >= y_lag - early)(lambda: y_event(k - y_lag))
        pl.when(k >= lag - early)(lambda: x_event(k - lag))
        pl.when(k >= p["last_x"])(lambda: last_x_event(k))
        pl.when(k < p["normal"])(lambda: early_work(k))
        pl.when(k >= ready)(lambda: late_work(k))
        extra_work(k)
        return carry

    lax.fori_loop(0, p["total"], one_slot, 0)
    target_copy.wait()
    for kind, index in p["tail"][:-1]:
        layer, y = extra_of(jnp.int32(kind))
        multiply(layer, y, turned(index), kind == 0)
    kind, index = p["tail"][-1]
    layer, y = extra_of(jnp.int32(kind))
    whole(layer, y, turned(index), kind == 0)
    exact = acc_ref[...] + product(layer, y, turned(index))
    out_ref[...] = exact.astype(jnp.bfloat16)
    error = exact - target_ref[...].astype(jnp.float32)
    error = error * error
    total = jnp.zeros((tokens, 128), jnp.float32)
    for k in range(columns // 128):
        total += error[:, k * 128 : (k + 1) * 128]
    share = jnp.zeros((8, 128), jnp.float32)
    for k in range(tokens // 8):
        share += total[k * 8 : (k + 1) * 8]

    fsdp = layers * 2
    members = 4 * fsdp
    spot = g * fsdp + f
    losses_ref[spot] = jnp.sum(share, axis=0, keepdims=True)

    def tell(j, carry):
        to = f + j
        to = jnp.where(to >= fsdp, to - fsdp, to)
        for i in range(4):

            @pl.when((i > 0) | (j > 0))
            def _():
                pltpu.make_async_remote_copy(
                    src_ref=losses_ref.at[spot],
                    dst_ref=losses_ref.at[spot],
                    send_sem=loss_sem.at[0],
                    recv_sem=loss_sem.at[1],
                    device_id=((g + i) % 4, to),
                    device_id_type=MESH,
                ).start()

        return carry

    lax.fori_loop(0, fsdp, tell, 0)

    def sent(layer, carry):
        up = inside(cl + 1) & (layer <= cl)
        down = inside(cl - 1) & (layer >= cl)
        own_up = up & (layer == cl)
        pl.when(own_up)(lambda: landed(some_rows(by_z), z_send.at[layers]))
        pl.when(down | (up & (layer != cl)))(
            lambda: landed(some_rows(by_z), z_send.at[layer])
        )
        return carry

    lax.fori_loop(0, layers, sent, 0)
    away = layers - 1
    landed(some_rows(away * by_y + own_y), y_send.at[0])
    landed(some_rows(away * (by_y + pieces - by_z) + pieces - own_y), x_send.at[0])
    landed(some_rows(away * pieces), core_send.at[cy])
    landed(some_rows(layers * pieces), core_send.at[1 - cy])
    others = losses_ref.at[pl.ds(0, members - 1)]
    landed(others, loss_sem.at[1])
    everyone = jnp.sum(losses_ref[...], axis=0)
    loss_ref[...] = jnp.sum(everyone, axis=1, keepdims=True) / (tokens * fsdp * columns)
    landed(others, loss_sem.at[0])


def per_device(fsdp, x, gain, codes, scales, outer, down, up, target):
    tokens, width = x.shape
    columns = up.shape[1]
    rows = codes.shape[0]
    layers = fsdp // 2
    pieces = rows // 2 // max(16, rows // 32)
    groups = min(4, rows // 128)
    hbm = pl.BlockSpec(memory_space=pltpu.HBM)
    dma = pltpu.SemaphoreType.DMA
    gain = gain.reshape(-1, 128)
    outer = outer.reshape(1, -1)
    operands = (x, gain, codes, scales, outer, down.T, up, target)
    operands = [pltpu.with_memory_space_constraint(a, pltpu.HBM) for a in operands]
    kv, loss = pl.pallas_call(
        functools.partial(kernel, layers, pieces, groups),
        out_shape=(
            pltpu.VMEM((tokens, columns), jnp.bfloat16),
            pltpu.VMEM((1, 1), jnp.float32),
        ),
        in_specs=[hbm] * 8,
        out_specs=(
            pl.BlockSpec(memory_space=pltpu.VMEM),
            pl.BlockSpec(memory_space=pltpu.VMEM),
        ),
        scratch_shapes=[
            pltpu.VMEM((tokens, width), jnp.bfloat16),
            pltpu.VMEM((width, columns), jnp.bfloat16),
            pltpu.VMEM((tokens, columns), jnp.float32),
            pltpu.VMEM((tokens, columns), jnp.bfloat16),
            pltpu.VMEM(down.shape[::-1], jnp.bfloat16),
            pltpu.VMEM(up.shape, jnp.bfloat16),
            pltpu.VMEM(gain.shape, jnp.bfloat16),
            pltpu.VMEM(codes.shape, jnp.int32),
            pltpu.VMEM(scales.shape, jnp.int32),
            pltpu.VMEM(outer.shape, jnp.int32),
            pltpu.VMEM((512, 512), jnp.bfloat16),
            pltpu.VMEM((4 * scales.shape[1], codes.shape[1]), jnp.bfloat16),
            pltpu.VMEM(codes.shape, jnp.float32),
            pltpu.VMEM((width // 128, 128), jnp.float32),
            pltpu.VMEM((tokens, down.shape[1]), jnp.float32),
            pltpu.VMEM((4 * fsdp, 1, 128), jnp.float32),
            dma((10 + groups,)),
            dma((layers + 1,)),
            dma((1,)),
            dma((1,)),
            dma((2,)),
            dma(((layers * 2 - 1) * pieces,)),
            dma((layers * 2 * groups,)),
            dma((2,)),
        ],
        compiler_params=pltpu.CompilerParams(
            collective_id=0, has_side_effects=True, vmem_limit_bytes=40 * 1024 * 1024
        ),
    )(*operands)
    return kv, loss.reshape(())


def solution(mesh):
    placed = (
        P(("grp", "fsdp"), None),
        P(),
        P("fsdp", None),
        P("fsdp", None),
        P("fsdp"),
        P(),
        P(),
        P(("grp", "fsdp"), None),
    )
    return jax.shard_map(
        functools.partial(per_device, mesh.shape["fsdp"]),
        mesh=mesh,
        in_specs=placed,
        out_specs=(P(("grp", "fsdp"), None), P()),
        check_vma=False,
    )
```
